32 devices in a mesh: seq: 8 (over z, x), tensor: 4 (over y, core).
Axes of the slice: x: 2, y: 2, z: 4, core: 2. Of those that a mesh axis runs over, the one named last changes fastest.
Arguments:
- hidden_in: bfloat16 [3072, 4096], P('seq', 'tensor'), may hold values from -6 to 6
- norm_gain: float32 [4096], replicated, may hold values from 0.5 to 1.5
- w_x: bfloat16 [4096, 8192], P('seq', 'tensor'), may hold values from -0.09375 to 0.09375
- w_z: bfloat16 [4096, 8192], P('seq', 'tensor'), may hold values from -0.09375 to 0.09375
- w_bc: bfloat16 [4096, 8, 256], P('seq', 'tensor'), may hold values from -0.09375 to 0.09375
- w_dt: bfloat16 [4096, 64], P('seq', 'tensor'), may hold values from -0.09375 to 0.09375
- dt_bias: float32 [64], P('tensor'), may hold values from -6 to -2
- decay_rate: float32 [64], P('tensor'), may hold values from 0.00032552084 to 8
- conv_x: float32 [4, 8192], P(None, 'tensor'), may hold values from -3 to 3
- conv_bc: float32 [4, 8, 256], P(None, 'tensor'), may hold values from -3 to 3
- conv_bias_x: float32 [8192], P('tensor'), may hold values from -3 to 3
- conv_bias_bc: float32 [8, 256], P('tensor'), may hold values from -3 to 3
- skip_d: float32 [64], P('tensor'), may hold values from 0.5 to 8
- out_gain: float32 [8192], P('tensor'), may hold values from 0.5 to 1.5
- w_out: bfloat16 [8192, 4096], P('tensor'), may hold values from -0.0625 to 0.0625
Outputs:
- layer_out: bfloat16 [3072, 4096], P('seq', 'tensor')
The draws below stay inside these ranges and needn't reach their ends.
All inputs are finite; a program needn't handle non-finite values.
Results may differ from the reference program's by a relative error of at most 0.0095.
Values may be sent and summed in bfloat16 or wider, within the bound.
A program may use at most 128 MiB of HBM per device.

```python
import math
import jax
import jax.numpy as jnp
from jax import lax

D = 4096
H = 64
P_SIZE = 128
N = 128
G = 8
KCONV = 4
SPAN = 128
DI = 8192
TOKENS = 3072


def shard_levels(stream_key, extent, cuts, smallest, largest):
    loudness, own = 1.0, jax.random.fold_in(stream_key, 6)
    for position, shards_of in cuts:
        draws = jnp.exp(jax.random.uniform(jax.random.fold_in(own, position), (shards_of,), jnp.float32, smallest / len(cuts), largest / len(cuts)))
        loudness = loudness * jnp.repeat(draws, extent[position] // shards_of).reshape([-1 if axis == position else 1 for axis in range(len(extent))])
    return loudness


def centred(stream_key, shape, deviation, most, split=(), dtype=jnp.bfloat16):
    gain = shard_levels(stream_key, shape, split, -0.22, 0.18) if split else 1.0
    entries = jax.random.normal(stream_key, shape, jnp.float32) * deviation * gain
    return jnp.minimum(jnp.maximum(entries, -most), most).astype(dtype)


def setup_inputs(seed: int = 0) -> dict:
    seeds = jax.random.split(jax.random.key(seed), 16)
    hidden_in = centred(seeds[0], (TOKENS, D), 1.0, 6.0, ((0, 8), (1, 4)))
    norm_gain = jnp.clip(1.0 + 0.1 * jax.random.normal(seeds[1], (D,), jnp.float32), 0.5, 1.5)
    w_x = centred(seeds[2], (D, DI), D ** -0.5, 0.09375, ((0, 8), (1, 4)))
    w_z = centred(seeds[3], (D, DI), D ** -0.5, 0.09375, ((0, 8), (1, 4)))
    w_bc = centred(seeds[4], (D, G, 2 * N), D ** -0.5, 0.09375, ((0, 8), (1, 4)))
    w_dt = centred(seeds[5], (D, H), D ** -0.5, 0.09375, ((0, 8), (1, 4)))
    dt_bias = jnp.clip(-6.0 + 4.0 * jax.random.uniform(seeds[6], (H,), jnp.float32) ** shard_levels(seeds[6], (H,), ((0, 4),), -0.2, 0.2), -6.0, -2.0)
    decay_rate = jnp.clip(jnp.exp(math.log(8.0) - 10.109526 * jax.random.uniform(seeds[7], (H,), jnp.float32) ** shard_levels(seeds[7], (H,), ((0, 4),), -0.2, 0.2)), 0.00032552084, 8.0)
    conv_x = centred(seeds[8], (KCONV, DI), KCONV ** -0.5, 3.0, ((1, 4),), jnp.float32)
    conv_bc = centred(seeds[9], (KCONV, G, 2 * N), KCONV ** -0.5, 3.0, ((1, 4),), jnp.float32)
    conv_bias_x = centred(seeds[10], (DI,), 0.5, 3.0, ((0, 4),), jnp.float32)
    conv_bias_bc = centred(seeds[11], (G, 2 * N), 0.5, 3.0, ((0, 4),), jnp.float32)
    skip_d = jnp.clip(jnp.exp(math.log(8.0) - 2.7725887 * jax.random.uniform(seeds[12], (H,), jnp.float32) ** shard_levels(seeds[12], (H,), ((0, 4),), -0.2, 0.2)), 0.5, 8.0)
    out_gain = jnp.clip(1.0 + 0.1 * jax.random.normal(seeds[13], (DI,), jnp.float32), 0.5, 1.5)
    w_out = centred(seeds[14], (DI, D), DI ** -0.5, 0.0625, ((0, 4),))
    return {"hidden_in": hidden_in, "norm_gain": norm_gain, "w_x": w_x, "w_z": w_z, "w_bc": w_bc, "w_dt": w_dt, "dt_bias": dt_bias, "decay_rate": decay_rate, "conv_x": conv_x, "conv_bc": conv_bc, "conv_bias_x": conv_bias_x, "conv_bias_bc": conv_bias_bc, "skip_d": skip_d, "out_gain": out_gain, "w_out": w_out}


epsilon = 1e-05

def rms_scale(values, norm_weight):
    return values * lax.rsqrt(lax.optimization_barrier(jnp.mean(values * values, axis=-1, keepdims=True)) + epsilon) * norm_weight

def causal_conv(padded, weight, bias_row):
    tap_count = weight.shape[0]
    out_length = padded.shape[0] - tap_count + 1
    running = bias_row.astype(jnp.float32)
    for k in range(tap_count):
        running = running + weight[k].astype(jnp.float32) * padded[k:k + out_length].astype(jnp.float32)
    return jax.nn.silu(running).astype(jnp.bfloat16)

def span_terms(x_blocks, b_blocks, c_blocks, log_decay, dt_blocks):
    cum_decay = jnp.cumsum(log_decay, axis=1)
    scores = jnp.einsum('ctgn,csgn->cgts', c_blocks.astype(jnp.float32), b_blocks.astype(jnp.float32))
    length = x_blocks.shape[1]
    causal_mask = lax.broadcasted_iota(jnp.int32, (length, length), 0) >= lax.broadcasted_iota(jnp.int32, (length, length), 1)
    cum_rows = jnp.transpose(cum_decay, (0, 2, 3, 1))
    decay_gap = cum_rows[..., :, None] - cum_rows[..., None, :]
    decay_mat = jnp.where(causal_mask, jnp.exp(jnp.where(causal_mask, decay_gap, 0.0)), 0.0)
    dt_cols = jnp.transpose(dt_blocks, (0, 2, 3, 1))[..., None, :]
    mix_weight = (scores[:, :, None] * decay_mat * dt_cols).astype(jnp.bfloat16)
    intra_out = jnp.einsum('cgkts,csgkp->ctgkp', mix_weight.astype(jnp.float32), x_blocks.astype(jnp.float32))
    tail_decay = jnp.exp(cum_decay[:, -1:] - cum_decay) * dt_blocks
    scaled = (x_blocks.astype(jnp.float32) * tail_decay[..., None]).astype(jnp.bfloat16)
    fresh_state = jnp.einsum('csgkp,csgn->cgkpn', scaled.astype(jnp.float32), b_blocks.astype(jnp.float32))
    return (cum_decay, intra_out, fresh_state)

def reference(hidden_in, norm_gain, w_x, w_z, w_bc, w_dt, dt_bias, decay_rate, conv_x, conv_bc, conv_bias_x, conv_bias_bc, skip_d, out_gain, w_out):
    per_group = H // G
    span_count = TOKENS // SPAN
    rim_rows = KCONV - 1
    normed = rms_scale(hidden_in.astype(jnp.float32), norm_gain).astype(jnp.bfloat16)
    proj_x = jnp.dot(normed, w_x, preferred_element_type=jnp.float32).astype(jnp.bfloat16)
    gate_z = jnp.dot(normed, w_z, preferred_element_type=jnp.float32).astype(jnp.bfloat16)
    proj_bc = jnp.dot(normed, w_bc.reshape(D, G * 2 * N), preferred_element_type=jnp.float32).astype(jnp.bfloat16).reshape(TOKENS, G, 2 * N)
    dt_vals = jax.nn.softplus(jnp.dot(normed, w_dt, preferred_element_type=jnp.float32) + dt_bias)
    x_conv = causal_conv(jnp.concatenate([jnp.zeros((rim_rows, DI), jnp.bfloat16), proj_x], axis=0), conv_x, conv_bias_x)
    bc_conv = causal_conv(jnp.concatenate([jnp.zeros((rim_rows, G, 2 * N), jnp.bfloat16), proj_bc], axis=0), conv_bc, conv_bias_bc)
    x_blocks = x_conv.reshape(span_count, SPAN, G, per_group, P_SIZE)
    b_blocks = bc_conv[..., :N].reshape(span_count, SPAN, G, N)
    c_blocks = bc_conv[..., N:].reshape(span_count, SPAN, G, N)
    log_decay = (-dt_vals * decay_rate).reshape(span_count, SPAN, G, per_group)
    dt_blocks = dt_vals.reshape(span_count, SPAN, G, per_group)
    skip_heads = skip_d.reshape(G, per_group)[..., None]

    def span_step(state_in, block_item):
        x_block, b_block, c_block, log_block, dt_block = [piece[None] for piece in block_item]
        cum_decay, intra_out, fresh_state = span_terms(x_block, b_block, c_block, log_block, dt_block)
        inter_out = jnp.exp(cum_decay)[..., None] * jnp.einsum('ctgn,gkpn->ctgkp', c_block.astype(jnp.float32), state_in, precision=lax.Precision.HIGHEST)
        ssm_out = intra_out + inter_out + skip_heads * x_block.astype(jnp.float32)
        state_next = jnp.exp(cum_decay[0, -1])[..., None, None] * state_in + fresh_state[0]
        return (state_next, ssm_out[0])
    start_state = jnp.zeros((G, per_group, P_SIZE, N), jnp.float32)
    final_state, ssm_out = lax.scan(span_step, start_state, (x_blocks, b_blocks, c_blocks, log_decay, dt_blocks))
    ssm_out = ssm_out.reshape(TOKENS, DI)
    gated_out = ssm_out * jax.nn.silu(gate_z.astype(jnp.float32))
    grouped = gated_out.reshape(TOKENS, G, DI // G)
    normed_y = rms_scale(grouped, out_gain.reshape(G, DI // G)).reshape(TOKENS, DI).astype(jnp.bfloat16)
    mixed = jnp.dot(normed_y, w_out, preferred_element_type=jnp.float32)
    return (hidden_in.astype(jnp.float32) + mixed).astype(jnp.bfloat16)
```

```python
import functools

import jax
import jax.numpy as jnp
from jax import lax
from jax.experimental import pallas as pl
from jax.experimental.pallas import tpu as pltpu
from jax.sharding import Mesh, PartitionSpec as P

MESH = pl.DeviceIdType.MESH
SPAN = 128
RING_LIMIT = 8


epsilon = 1e-05


def rms_scale(values, norm_weight):
    return (
        values
        * lax.rsqrt(jnp.mean(values * values, axis=-1, keepdims=True) + epsilon)
        * norm_weight
    )


def causal_conv(padded, weight, bias_row):
    tap_count = weight.shape[0]
    out_length = padded.shape[0] - tap_count + 1
    running = bias_row
    for k in range(tap_count):
        running = running + weight[k] * padded[k : k + out_length].astype(jnp.float32)
    return jax.nn.silu(running).astype(jnp.bfloat16)


def span_terms(x_blocks, b_blocks, c_blocks, log_decay, dt_blocks):
    cum_decay = jnp.cumsum(log_decay, axis=1)
    scores = jnp.einsum("ctgn,csgn->cgts", c_blocks, b_blocks, preferred_element_type=jnp.float32)
    length = x_blocks.shape[1]
    causal_mask = lax.broadcasted_iota(jnp.int32, (length, length), 0) >= lax.broadcasted_iota(
        jnp.int32, (length, length), 1
    )
    cum_rows = jnp.transpose(cum_decay, (0, 2, 3, 1))
    decay_gap = cum_rows[..., :, None] - cum_rows[..., None, :]
    decay_mat = jnp.where(causal_mask, jnp.exp(jnp.where(causal_mask, decay_gap, 0.0)), 0.0)
    dt_cols = jnp.transpose(dt_blocks, (0, 2, 3, 1))[..., None, :]
    mix_weight = (scores[:, :, None] * decay_mat * dt_cols).astype(jnp.bfloat16)
    intra_out = jnp.einsum(
        "cgkts,csgkp->ctgkp", mix_weight, x_blocks, preferred_element_type=jnp.float32
    )
    tail_decay = jnp.exp(cum_decay[:, -1:] - cum_decay) * dt_blocks
    scaled = (x_blocks.astype(jnp.float32) * tail_decay[..., None]).astype(jnp.bfloat16)
    fresh_state = jnp.einsum(
        "csgkp,csgn->cgkpn", scaled, b_blocks, preferred_element_type=jnp.float32
    )
    return (cum_decay, intra_out, fresh_state)


def shifted(block, axis, distance):
    count = lax.axis_size(axis)
    return lax.ppermute(block, axis, [(i, (i + distance) % count) for i in range(count)])


def passed_along(block, axis, distance):
    devices = range(lax.axis_size(axis))
    return lax.ppermute(block, axis, [(i - distance, i) for i in devices if i - distance in devices])


def swapped(block, axis, bit):
    return lax.ppermute(block, axis, [(i, i ^ bit) for i in range(lax.axis_size(axis))])


def ring_pieces(own, axis):
    count = lax.axis_size(axis)
    pieces = [(0, 0, own)]
    ahead, behind = own, own
    for step in range(1, (count - 1) // 2 + 1):
        ahead, behind = shifted(ahead, axis, 1), shifted(behind, axis, -1)
        pieces += [(step, 0, ahead), (count - step, 0, behind)]
    if count % 2 == 0:
        half = own.shape[0] // 2
        pieces += [
            (count // 2, 0, shifted(ahead[:half], axis, 1)),
            (count // 2, half, shifted(behind[half:], axis, -1)),
        ]
    return pieces


def carried_in(total_log, state):
    count, mine = lax.axis_size("outer"), lax.axis_index("outer")
    logs, states = lax.all_gather((total_log, state), "outer")

    def hop(position, running):
        longer = jnp.exp(logs[position])[..., None, None] * running + states[position]
        return jnp.where(position < mine, longer, running)

    return lax.fori_loop(0, count - 1, hop, jnp.zeros_like(state))


def gather_tokens(hidden_in):
    tensor, fold = lax.axis_size("tensor"), lax.axis_size("fold")
    rows, cols = hidden_in.shape
    pieces = [(0, 0, hidden_in)]
    bits = []
    bit = tensor // 2
    while bit > 1:
        bits.append(("tensor", bit))
        bit //= 2
    if fold > 1:
        bits.append(("fold", 1))
    if tensor > 1:
        bits.append(("tensor", 1))
    for axis, bit in bits:
        pieces += [
            (j ^ bit, k, swapped(part, axis, bit)) if axis == "tensor" else (j, k ^ bit, swapped(part, axis, bit))
            for j, k, part in list(pieces)
        ]
    full = jnp.zeros((tensor, rows * fold, cols), hidden_in.dtype)
    me_t, me_f = lax.axis_index("tensor"), lax.axis_index("fold")
    for j, k, part in pieces:
        full = lax.dynamic_update_slice(full, part[None], (me_t ^ j, (me_f ^ k) * rows, 0))
    return full


def scatter_sum(partial, rows, cols):
    tensor, fold = lax.axis_size("tensor"), lax.axis_size("fold")
    me_t, me_f = lax.axis_index("tensor"), lax.axis_index("fold")
    if tensor > 1:
        pairs = partial.reshape(fold * rows, tensor // 2, 2, cols)
        core = me_t % 2
        keep = lax.dynamic_index_in_dim(pairs, core, 2, keepdims=False)
        send = lax.dynamic_index_in_dim(pairs, 1 - core, 2, keepdims=False)
        keep = keep.astype(jnp.float32) + swapped(send.astype(jnp.bfloat16), "tensor", 1).astype(jnp.float32)
    else:
        keep = partial.reshape(fold * rows, 1, cols).astype(jnp.float32)

    def over_fold(value):
        if fold == 1:
            return value
        split = value.reshape(fold, rows, *value.shape[1:])
        mine = lax.dynamic_index_in_dim(split, me_f, 0, keepdims=False)
        other = lax.dynamic_index_in_dim(split, 1 - me_f, 0, keepdims=False)
        return mine + swapped(other.astype(jnp.bfloat16), "fold", 1).astype(jnp.float32)

    def over_high(value):
        count = tensor // 2
        bit = tensor // 2
        while count > 1:
            split = value.reshape(value.shape[0], 2, count // 2, value.shape[-1])
            top = (me_t // bit) % 2
            mine = lax.dynamic_index_in_dim(split, top, 1, keepdims=False)
            other = lax.dynamic_index_in_dim(split, 1 - top, 1, keepdims=False)
            value = mine + swapped(other.astype(jnp.bfloat16), "tensor", bit).astype(jnp.float32)
            count, bit = count // 2, bit // 2
        return value

    half = cols // 2
    first = over_high(over_fold(keep[..., :half]))
    second = over_fold(over_high(keep[..., half:]))
    return jnp.concatenate([first.reshape(rows, half), second.reshape(rows, cols - half)], axis=1)


def local(
    hidden_in,
    norm_gain,
    w_x,
    w_z,
    w_bc,
    w_dt,
    dt_bias,
    decay_rate,
    conv_x,
    conv_bc,
    conv_bias_x,
    conv_bias_bc,
    skip_d,
    out_gain,
    w_out,
):
    fold = lax.axis_size("fold")
    me_f = lax.axis_index("fold")
    me_o = lax.axis_index("outer")
    outer = lax.axis_size("outer")

    def part(value, axis, which=None):
        size = value.shape[axis] // fold
        which = me_f if which is None else which
        return lax.dynamic_slice_in_dim(value, which * size, size, axis)

    depth = w_x.shape[0]
    groups = w_bc.shape[1] // fold
    bc_width = w_bc.shape[2]
    bc_flat = w_bc.reshape(depth, w_bc.shape[1] * bc_width)
    state_dim = bc_width // 2
    head_count = decay_rate.shape[0] // fold
    inner_width = w_x.shape[1] // fold
    head_dim = inner_width // head_count
    per_group = head_count // groups

    def weights(which):
        side = jnp.concatenate([part(bc_flat, 1, which), part(w_dt, 1, which)], axis=1)
        return [jnp.concatenate([part(w_x, 1, which), side], axis=1), part(w_z, 1, which)]

    own = weights(me_f)
    other = [swapped(block, "fold", 1) for block in weights(1 - me_f)] if fold > 1 else []
    gathered = gather_tokens(hidden_in)
    blocks, row_count, width = gathered.shape
    values = gathered.astype(jnp.float32)
    scale = lax.rsqrt(jnp.mean(values * values, axis=(0, 2), keepdims=True) + epsilon)
    normed = (values * scale * norm_gain.reshape(blocks, 1, width)).astype(jnp.bfloat16)
    per_block = max(width // depth, 1)
    if outer <= RING_LIMIT:
        normed = normed.reshape(blocks, row_count, per_block, width // per_block)
        normed = jnp.transpose(normed, (0, 2, 1, 3)).reshape(blocks * per_block, row_count, depth)
    else:
        normed = jnp.transpose(normed, (1, 0, 2)).reshape(row_count, blocks * width)
    rim_rows = conv_x.shape[0] - 1

    def projected(index):
        total = None
        if outer > RING_LIMIT:
            rows = lax.all_gather(own[index], "outer")
            if fold > 1:
                theirs = lax.all_gather(other[index], "outer")
                first, second = jnp.where(me_f == 0, rows, theirs), jnp.where(me_f == 0, theirs, rows)
                rows = jnp.stack([first, second], axis=1)
            rows = rows.reshape(normed.shape[1], own[index].shape[1])
            return jnp.dot(normed, rows, preferred_element_type=jnp.float32)
        for k, block in enumerate([own, other] if fold > 1 else [own]):
            for behind, offset, piece in ring_pieces(block[index], "outer"):
                owner = (me_o - behind + outer) % outer
                lhs = lax.dynamic_index_in_dim(normed, owner * fold + (me_f ^ k), 0, keepdims=False)
                lhs = lhs[:, offset : offset + piece.shape[0]]
                term = jnp.dot(lhs, piece, preferred_element_type=jnp.float32)
                total = term if total is None else total + term
        return total

    first = projected(0)
    proj_x = first[:, :inner_width].astype(jnp.bfloat16)
    side = first[:, inner_width:]
    dt_raw = side[:, groups * bc_width :]
    proj_bc = side[:, : groups * bc_width].astype(jnp.bfloat16)
    gate_z = projected(1).astype(jnp.bfloat16)
    edge_x, edge_bc = passed_along(
        (proj_x[row_count - rim_rows :], proj_bc[row_count - rim_rows :]), "outer", 1
    )
    padded_x = jnp.concatenate([edge_x, proj_x], axis=0)
    padded_bc = jnp.concatenate([edge_bc, proj_bc], axis=0)
    dt_vals = jax.nn.softplus(dt_raw + part(dt_bias, 0))
    x_conv = causal_conv(padded_x, part(conv_x, 1), part(conv_bias_x, 0))
    bc_conv = causal_conv(
        padded_bc,
        part(conv_bc, 1).reshape(conv_bc.shape[0], groups * bc_width),
        part(conv_bias_bc, 0).reshape(groups * bc_width),
    ).reshape(row_count, groups, bc_width)
    span_count = row_count // SPAN
    x_blocks = x_conv.reshape(span_count, SPAN, groups, per_group, head_dim)
    b_blocks = bc_conv[..., :state_dim].reshape(span_count, SPAN, groups, state_dim)
    c_blocks = bc_conv[..., state_dim:].reshape(span_count, SPAN, groups, state_dim)
    log_decay = (-dt_vals * part(decay_rate, 0)).reshape(span_count, SPAN, groups, per_group)
    dt_blocks = dt_vals.reshape(span_count, SPAN, groups, per_group)
    cum_decay, intra_out, fresh_state = span_terms(
        x_blocks, b_blocks, c_blocks, log_decay, dt_blocks
    )
    block_totals = cum_decay[:, -1]
    state = jnp.zeros((groups, per_group, head_dim, state_dim), jnp.float32)
    entering = []
    for i in range(span_count):
        entering.append(state)
        state = jnp.exp(block_totals[i])[..., None, None] * state + fresh_state[i]
    local_enter = jnp.stack(entering)
    before_log = jnp.cumsum(block_totals, axis=0) - block_totals
    total_log = jnp.sum(block_totals, axis=0)
    if outer > RING_LIMIT:
        incoming = carried_in(total_log, state)
    else:
        incoming = jnp.zeros_like(state)
        log_between = jnp.zeros_like(total_log)
        for distance in range(1, outer):
            arrived = passed_along(state, "outer", distance)
            incoming = incoming + jnp.exp(log_between)[..., None, None] * arrived
            log_between = log_between + passed_along(total_log, "outer", distance)
    enter_state = local_enter + jnp.exp(before_log)[..., None, None] * incoming[None]
    inter_out = jnp.exp(cum_decay)[..., None] * jnp.einsum(
        "ctgn,cgkpn->ctgkp", c_blocks, enter_state.astype(jnp.bfloat16), preferred_element_type=jnp.float32
    )
    skip_heads = part(skip_d, 0).reshape(groups, per_group)[..., None]
    ssm_out = (intra_out + inter_out + skip_heads * x_blocks.astype(jnp.float32)).reshape(
        row_count, inner_width
    )
    gated_out = ssm_out * jax.nn.silu(gate_z.astype(jnp.float32))
    grouped = gated_out.reshape(row_count, groups, inner_width // groups)
    normed_y = (
        rms_scale(grouped, part(out_gain, 0).reshape(groups, inner_width // groups))
        .reshape(row_count, inner_width)
        .astype(jnp.bfloat16)
    )
    partial = jnp.dot(normed_y, part(w_out, 0), preferred_element_type=jnp.float32)
    summed = scatter_sum(partial, *hidden_in.shape)
    return (hidden_in.astype(jnp.float32) + summed).astype(jnp.bfloat16)


def wait_in(dst, sem, me):
    pltpu.make_async_remote_copy(
        src_ref=dst, dst_ref=dst, send_sem=sem, recv_sem=sem, device_id=me, device_id_type=MESH
    ).wait_recv()


def wait_out(src, sem, me):
    pltpu.make_async_remote_copy(
        src_ref=src, dst_ref=src, send_sem=sem, recv_sem=sem, device_id=me, device_id_type=MESH
    ).wait_send()


def push(src, dst, send_sem, recv_sem, device):
    pltpu.make_async_remote_copy(
        src_ref=src, dst_ref=dst, send_sem=send_sem, recv_sem=recv_sem, device_id=device, device_id_type=MESH
    ).start()


def greet(partners):
    barrier = pltpu.get_barrier_semaphore()
    for device in partners:
        pl.semaphore_signal(barrier, inc=1, device_id=device, device_id_type=MESH)
    pl.semaphore_wait(barrier, len(partners))


def guarded(condition, action):
    if condition is None:
        action()
    else:
        pl.when(condition)(action)


def as_column(row):
    return jnp.transpose(jnp.broadcast_to(row[0:1], (row.shape[1], row.shape[1])))[:, 0:1]


def as_row(column):
    return jnp.transpose(jnp.broadcast_to(column, (column.shape[0], column.shape[0])))[0:8]


def project_kernel(
    dims,
    x_ref, gain_ref, wx_ref, wz_ref, wbc_ref, wdt_ref,
    xz_ref, bc_ref, dt_ref,
    tok, wgt, side, acc, dtw, sums, bcs,
    own_sem, tok_recv, z_up, z_down, x_send, y_send, core_send,
    w_send, w_recv, d_send, d_recv, s_send, s_recv, b_send, b_recv,
):
    ns, nt = dims
    nz = ns // 2
    rows, feats = x_ref.shape
    depth = wx_ref.shape[0]
    width = wx_ref.shape[1] // ns
    s, t = lax.axis_index("seq"), lax.axis_index("tensor")
    z, x = s // 2, s % 2
    y, core = t // 2, t % 2
    me = (s, t)
    sx = 2 * z + 1 - x
    ty = 2 * (1 - y) + core
    tc = 2 * y + 1 - core
    tyc = 2 * (1 - y) + 1 - core
    half_w = ns // 2
    main = 2 * width
    lanes = 128

    partners = [(lax.rem(s + i, ns), t) for i in range(1, ns)]
    partners += [(s, lax.rem(t + i, nt)) for i in range(1, nt)]
    greet(partners)

    devices_per_group = ns // (wbc_ref.shape[1] // (2 * lanes))

    def weight_parts(dest):
        group, half = dest // devices_per_group, dest % 2
        column = pl.multiple_of(dest * width, lanes)
        third = pl.multiple_of((group * 2 + half) * lanes, lanes)
        return [
            (wx_ref.at[:, pl.ds(column, width)], 0, width),
            (wz_ref.at[:, pl.ds(column, width)], width, width),
            (wbc_ref.at[:, pl.ds(third, lanes)], main, lanes),
        ]

    def send_weights(dz, flip):
        def go():
            dest = 2 * (z + dz) + (1 - x if flip else x)
            for src, lane, size in weight_parts(dest):
                push(src, wgt.at[s, :, pl.ds(lane, size)], w_send.at[dest], w_recv.at[s], (dest, t))
            push(wdt_ref.at[dest], dtw.at[s], d_send.at[dest], d_recv.at[s], (dest, t))

        inside(dz, go)

    def inside(dz, action):
        if dz == 0:
            action()
        elif dz > 0:
            pl.when(z + dz < nz)(action)
        else:
            pl.when(z + dz >= 0)(action)

    own_copies = [
        pltpu.make_async_copy(src, wgt.at[s, :, pl.ds(lane, size)], own_sem.at[i])
        for i, (src, lane, size) in enumerate(weight_parts(s))
    ]
    own_copies.append(pltpu.make_async_copy(wdt_ref.at[s], dtw.at[s], own_sem.at[3]))
    for copy in own_copies:
        copy.start()
    send_weights(1, False)
    send_weights(-1, False)

    for r in range(0, rows, lanes):
        values = x_ref[r : r + lanes, :].astype(jnp.float32)
        sums[t, :, r : r + lanes] = as_row(jnp.sum(values * values, axis=1, keepdims=True))
    for i in range(1, nt):
        peer = lax.rem(t + i, nt)
        push(sums.at[t], sums.at[t], s_send.at[peer], s_recv.at[t], (s, peer))
    for i in range(1, nt):
        peer = lax.rem(t + i, nt)
        wait_in(sums.at[peer], s_recv.at[peer], me)
    gain = gain_ref[pl.ds(t, 1), :]
    for r in range(0, rows, lanes):
        total = sums[0, :, r : r + lanes]
        for i in range(1, nt):
            total = total + sums[i, :, r : r + lanes]
        scale = as_column(lax.rsqrt(total * (1.0 / (nt * feats)) + epsilon))
        values = x_ref[r : r + lanes, :].astype(jnp.float32)
        tok[s, t, r : r + lanes, :] = (values * scale * gain).astype(jnp.bfloat16)

    def send_tok(si, ti, send_sem, device):
        push(tok.at[si, ti], tok.at[si, ti], send_sem, tok_recv.at[si, ti], device)

    def wait_tok(si, ti):
        wait_in(tok.at[si, ti], tok_recv.at[si, ti], me)

    def from_z(dz):
        zb = z + dz
        block = 2 * zb + x
        if dz != 0:
            wait_tok(block, t)
        if dz <= 0:
            pl.when(z < nz - 1)(lambda: send_tok(block, t, z_up.at[zb], (s + 2, t)))
        if dz >= 0:
            pl.when(z > 0)(lambda: send_tok(block, t, z_down.at[zb], (s - 2, t)))
        send_tok(block, t, x_send.at[zb], (sx, t))
        send_tok(block, t, y_send.at[block], (s, ty))
        send_tok(block, t, core_send.at[0, block], (s, tc))

    def from_x(dz):
        block = 2 * (z + dz) + 1 - x
        wait_tok(block, t)
        send_tok(block, t, y_send.at[block], (s, ty))
        send_tok(block, t, core_send.at[0, block], (s, tc))

    def from_y(dz):
        for flip in (x, 1 - x):
            block = 2 * (z + dz) + flip
            wait_tok(block, ty)
            send_tok(block, ty, core_send.at[1, block], (s, tc))

    def from_core(dz, which):
        for flip in (x, 1 - x):
            wait_tok(2 * (z + dz) + flip, which)

    steps = [0]
    for k in range(1, nz):
        steps += [-k, k]

    from_z(0)
    send_weights(0, True)
    for k in range(1, nz):
        for dz in (-k, k):
            inside(dz, lambda dz=dz: from_z(dz))
        for dz in (-k, k):
            send_weights(dz, True)
            if k + 1 < nz:
                send_weights(dz + (1 if dz > 0 else -1), False)
        for dz in ([0] if k == 1 else [-(k - 1), k - 1]):
            inside(dz, lambda dz=dz: from_x(dz))
        if k == 2:
            from_y(0)
    for dz in (-(nz - 1), nz - 1):
        inside(dz, lambda dz=dz: from_x(dz))
    for copy in own_copies:
        copy.wait()

    def weight_ready(source):
        @pl.when(source != s)
        def _():
            wait_in(wgt.at[source], w_recv.at[source], me)
            wait_in(dtw.at[source], d_recv.at[source], me)

        side[source, :, 0:lanes] = wgt[source, :, main:]
        short = dtw[source].astype(jnp.float32)
        padded = jnp.concatenate([short, jnp.zeros((lanes - short.shape[0], depth), jnp.float32)], axis=0)
        side[source, :, lanes:] = jnp.transpose(padded).astype(jnp.bfloat16)

    def product(block, part, put):
        first = part * (nt // 2)
        lhs = jnp.concatenate([tok[block, first + i] for i in range(nt // 2)], axis=1)
        source = pl.ds(part * half_w, half_w)
        for n in range(0, main + 2 * lanes, 256):
            if n < main:
                rhs = wgt[source, :, n : n + 256]
            else:
                rhs = side[source, :, n - main : n - main + 256]
            rhs = rhs.reshape(half_w * depth, 256)
            put(n, jnp.dot(lhs, rhs, preferred_element_type=jnp.float32))

    for dz in steps:
        inside(dz, lambda dz=dz: from_core(dz, tc))

    @pl.loop(0, half_w)
    def _(i):
        weight_ready(y * half_w + i)

    @pl.loop(0, ns)
    def _(block):
        def put(n, value):
            acc[block, :, n : n + 256] = value

        product(block, y, put)

    @pl.loop(0, half_w)
    def _(i):
        weight_ready((1 - y) * half_w + i)

    def finish(block):
        def put(n, value):
            value = acc[block, :, n : n + 256] + value
            if n < main:
                xz_ref[block, :, n : n + 256] = value.astype(jnp.bfloat16)
            else:
                bcs[x, block] = value[:, 0:lanes].astype(jnp.bfloat16)
                dt_ref[block] = value[:, lanes:]

        product(block, 1 - y, put)
        push(bcs.at[x, block], bcs.at[x, block], b_send.at[block], b_recv.at[block], (sx, t))

    for dz in steps[1:]:
        inside(dz, lambda dz=dz: from_y(dz))
    for dz in steps:

        def group(dz=dz):
            from_core(dz, tyc)
            for flip in (x, 1 - x):
                finish(2 * (z + dz) + flip)

        inside(dz, group)

    @pl.loop(0, ns)
    def _(block):
        wait_in(bcs.at[1 - x, block], b_recv.at[block], me)
        wait_out(bcs.at[x, block], b_send.at[block], me)
        bc_ref[0, block] = bcs[0, block]
        bc_ref[1, block] = bcs[1, block]
        wait_out(tok.at[block, t], y_send.at[block], me)
        wait_out(tok.at[block, t], core_send.at[0, block], me)
        wait_out(tok.at[block, t], core_send.at[1, block], me)

        @pl.when(block != s)
        def _():
            wait_out(wgt.at[block], w_send.at[block], me)
            wait_out(dtw.at[block], d_send.at[block], me)

    for dz in steps:

        def drain(dz=dz):
            zb = z + dz
            if dz <= 0:
                pl.when(z < nz - 1)(lambda: wait_out(tok.at[0, 0], z_up.at[zb], me))
            if dz >= 0:
                pl.when(z > 0)(lambda: wait_out(tok.at[0, 0], z_down.at[zb], me))
            wait_out(tok.at[0, 0], x_send.at[zb], me)

        inside(dz, drain)
    for i in range(1, nt):
        wait_out(sums.at[t], s_send.at[lax.rem(t + i, nt)], me)


def mix_kernel(
    dims,
    xz_ref, bc_ref, dt_ref, convx_ref, convbc_ref, head_ref, gain_ref, wout_ref, hidden_ref,
    out_ref,
    tail, state, gated, norms, landed, norms_in, wout, send_one, recv_one, send_two, recv_two,
    w_sem, g_send, g_recv, n_send, n_recv, one_send, one_recv, two_send, two_recv,
):
    ns, nt, heads = dims
    rows = xz_ref.shape[1]
    width = xz_ref.shape[2] // 2
    head_dim = width // heads
    lanes = 128
    s, t = lax.axis_index("seq"), lax.axis_index("tensor")
    me = (s, t)
    y, core = t // 2, t % 2
    ty = 2 * (1 - y) + core
    tc = 2 * y + 1 - core
    tyc = 2 * (1 - y) + 1 - core
    groups = convbc_ref.shape[0]
    group_devices = ns // groups
    group_width = group_devices * width

    fetch = pltpu.make_async_copy(wout_ref, wout, w_sem)
    fetch.start()
    partners = [(lax.rem(s + i, ns), t) for i in range(1, ns)]
    partners += [(s, tc), (s, ty)]
    greet(partners)

    tail[...] = jnp.zeros_like(tail)
    state[...] = jnp.zeros_like(state)
    column = pl.multiple_of(s * width, lanes)
    taps_x = convx_ref[:, pl.ds(column, width)]
    group = s // group_devices
    taps_bc = convbc_ref[group]
    tap_count = taps_x.shape[0] - 1
    dt_bias = head_ref[0, pl.ds(s, 1), :]
    decay = head_ref[1, pl.ds(s, 1), :]
    skip = head_ref[2, pl.ds(s, 1), :]
    out_gain = gain_ref[:, pl.ds(column, width)]
    span_rows = lax.broadcasted_iota(jnp.int32, (SPAN, SPAN), 0)
    span_cols = lax.broadcasted_iota(jnp.int32, (SPAN, SPAN), 1)
    causal = span_rows >= span_cols
    lower = jnp.where(causal, 1.0, 0.0)

    def conv(previous, current, taps):
        padded = jnp.concatenate([previous, current], axis=0)
        running = taps[tap_count : tap_count + 1]
        for k in range(tap_count):
            start = 8 - (tap_count - 1) + k
            running = running + taps[k : k + 1] * padded[start : start + SPAN]
        return (running * jax.nn.sigmoid(running)).astype(jnp.bfloat16)

    def span(block, r):
        x_raw = xz_ref[block, r : r + SPAN, 0:width].astype(jnp.float32)
        b_raw = bc_ref[0, block, r : r + SPAN, :].astype(jnp.float32)
        c_raw = bc_ref[1, block, r : r + SPAN, :].astype(jnp.float32)
        bc_raw = jnp.concatenate([b_raw, c_raw], axis=1)
        x_conv = conv(tail[:, 0:width], x_raw, taps_x)
        bc_conv = conv(tail[:, width:], bc_raw, taps_bc)
        tail[:, 0:width] = x_raw[SPAN - 8 :]
        tail[:, width:] = bc_raw[SPAN - 8 :]
        b_conv, c_conv = bc_conv[:, 0:lanes], bc_conv[:, lanes:]
        raw = dt_ref[block, r : r + SPAN, :] + dt_bias
        dt = jnp.maximum(raw, 0.0) + jnp.log1p(jnp.exp(-jnp.abs(raw)))
        cum = jnp.dot(lower, -dt * decay, precision=lax.Precision.HIGHEST, preferred_element_type=jnp.float32)
        cum_t = jnp.transpose(cum)
        dt_t = jnp.transpose(dt)
        scores = lax.dot_general(c_conv, b_conv, (((1,), (1,)), ((), ())), preferred_element_type=jnp.float32)
        b_t = jnp.transpose(b_conv.astype(jnp.float32)).astype(jnp.bfloat16)
        squares = None
        for h in range(heads):
            x_h = x_conv[:, h * head_dim : (h + 1) * head_dim]
            x_f = x_h.astype(jnp.float32)
            cum_h = cum[:, h : h + 1]
            gap = jnp.where(causal, cum_h - cum_t[h : h + 1, :], -jnp.inf)
            mix = (scores * jnp.exp(gap) * dt_t[h : h + 1, :]).astype(jnp.bfloat16)
            value = jnp.dot(mix, x_h, preferred_element_type=jnp.float32)
            last = cum[SPAN - 1 : SPAN, h : h + 1]
            scaled = (x_f * (jnp.exp(last - cum_h) * dt[:, h : h + 1])).astype(jnp.bfloat16)
            entering = state[h]
            value = value + jnp.exp(cum_h) * jnp.dot(
                c_conv, entering.astype(jnp.bfloat16), preferred_element_type=jnp.float32
            )
            state[h] = jnp.exp(last) * entering + jnp.dot(b_t, scaled, preferred_element_type=jnp.float32)
            value = value + skip[:, h : h + 1] * x_f
            start = width + h * head_dim
            gate = xz_ref[block, r : r + SPAN, start : start + head_dim].astype(jnp.float32)
            value = value * (gate * jax.nn.sigmoid(gate))
            square = jnp.sum(value * value, axis=1, keepdims=True)
            squares = square if squares is None else squares + square
            gain = out_gain[:, h * head_dim : (h + 1) * head_dim]
            gated[block, r : r + SPAN, h * head_dim : (h + 1) * head_dim] = (value * gain).astype(jnp.bfloat16)
        norms[block, :, r : r + SPAN] = as_row(squares)

    @pl.loop(0, ns)
    def _(block):
        for r in range(0, rows, SPAN):
            span(block, r)

        @pl.when(block != s)
        def _():
            push(gated.at[block], landed.at[s], g_send.at[block], g_recv.at[s], (block, t))
            push(norms.at[block], norms_in.at[s], n_send.at[block], n_recv.at[s], (block, t))

        @pl.when(block == s)
        def _():
            landed[s] = gated[block]
            norms_in[s] = norms[block]

    fetch.wait()
    for i in range(1, ns):
        source = lax.rem(s + i, ns)
        wait_in(landed.at[source], g_recv.at[source], me)
        wait_in(norms_in.at[source], n_recv.at[source], me)

    scales, lhs = [], []
    for g in range(groups):
        total = norms_in[g * group_devices]
        for i in range(1, group_devices):
            total = total + norms_in[g * group_devices + i]
        rate = lax.rsqrt(total * (1.0 / group_width) + epsilon)
        scales.append(
            jnp.concatenate([as_column(rate[:, r : r + lanes]) for r in range(0, rows, lanes)], axis=0)
        )
        lhs.append(jnp.concatenate([landed[g * group_devices + i] for i in range(group_devices)], axis=1))

    cols = hidden_ref.shape[1]
    chunk = cols // 2

    def partial(owner, c):
        column = pl.multiple_of(owner * cols + c * chunk, lanes)
        total = None
        for g in range(groups):
            weights = wout[g * group_width : (g + 1) * group_width, pl.ds(column, chunk)]
            term = scales[g] * jnp.dot(lhs[g], weights, preferred_element_type=jnp.float32)
            total = term if total is None else total + term
        return total

    def to_core(slot, owner, c):
        send_one[slot, c] = partial(owner, c).astype(jnp.bfloat16)
        push(send_one.at[slot, c], recv_one.at[slot, c], one_send.at[slot, c], one_recv.at[slot, c], (s, tc))

    for c in range(2):
        to_core(0, tyc, c)
        mine = partial(ty, c)
        wait_in(recv_one.at[0, c], one_recv.at[0, c], me)
        send_two[c] = (mine + recv_one[0, c].astype(jnp.float32)).astype(jnp.bfloat16)
        push(send_two.at[c], recv_two.at[c], two_send.at[c], two_recv.at[c], (s, ty))
    for c in range(2):
        to_core(1, tc, c)
    for c in range(2):
        mine = partial(t, c)
        wait_in(recv_one.at[1, c], one_recv.at[1, c], me)
        mine = mine + recv_one[1, c].astype(jnp.float32)
        mine = mine + hidden_ref[:, c * chunk : (c + 1) * chunk].astype(jnp.float32)
        wait_in(recv_two.at[c], two_recv.at[c], me)
        out_ref[:, c * chunk : (c + 1) * chunk] = (mine + recv_two[c].astype(jnp.float32)).astype(jnp.bfloat16)

    for i in range(1, ns):
        dest = lax.rem(s + i, ns)
        wait_out(gated.at[dest], g_send.at[dest], me)
        wait_out(norms.at[dest], n_send.at[dest], me)
    for c in range(2):
        for slot in range(2):
            wait_out(send_one.at[slot, c], one_send.at[slot, c], me)
        wait_out(send_two.at[c], two_send.at[c], me)


def spread_heads(ns, nt, *args):
    (hidden_in, norm_gain, w_x, w_z, w_bc, w_dt, dt_bias, decay_rate,
     conv_x, conv_bc, conv_bias_x, conv_bias_bc, skip_d, out_gain, w_out) = args
    rows, feats = hidden_in.shape
    depth, columns = w_x.shape
    width = columns // ns
    heads = decay_rate.shape[0] // ns
    groups, bc_width = w_bc.shape[1], w_bc.shape[2]
    state_dim = bc_width // 2
    head_dim = width // heads
    flat_bc = w_bc.reshape(depth, groups * bc_width)
    dt_rows = jnp.transpose(w_dt).reshape(ns, heads, depth)
    dt_rows = jnp.pad(dt_rows, ((0, 0), (0, 16 - heads), (0, 0)))
    anyw = pl.BlockSpec(memory_space=pl.ANY)
    vmem = pl.BlockSpec(memory_space=pltpu.VMEM)
    dma = pltpu.SemaphoreType.DMA
    total_width = 2 * width + 256
    xz, bc, dt = pl.pallas_call(
        functools.partial(project_kernel, (ns, nt)),
        out_shape=(
            jax.ShapeDtypeStruct((ns, rows, 2 * width), jnp.bfloat16),
            jax.ShapeDtypeStruct((2, ns, rows, 128), jnp.bfloat16),
            jax.ShapeDtypeStruct((ns, rows, 128), jnp.float32),
        ),
        in_specs=[vmem, vmem, anyw, anyw, anyw, anyw],
        out_specs=(vmem, vmem, vmem),
        scratch_shapes=[
            pltpu.VMEM((ns, nt, rows, feats), jnp.bfloat16),
            pltpu.VMEM((ns, depth, 2 * width + 128), jnp.bfloat16),
            pltpu.VMEM((ns, depth, 256), jnp.bfloat16),
            pltpu.VMEM((ns, rows, total_width), jnp.float32),
            pltpu.VMEM((ns, 16, depth), jnp.bfloat16),
            pltpu.VMEM((nt, 8, rows), jnp.float32),
            pltpu.VMEM((2, ns, rows, 128), jnp.bfloat16),
            dma((4,)), dma((ns, nt)), dma((ns // 2,)), dma((ns // 2,)), dma((ns // 2,)), dma((ns,)), dma((2, ns)),
            dma((ns,)), dma((ns,)), dma((ns,)), dma((ns,)), dma((nt,)), dma((nt,)), dma((ns,)), dma((ns,)),
        ],
        compiler_params=pltpu.CompilerParams(
            collective_id=0, has_side_effects=True, vmem_limit_bytes=62 * 1024 * 1024
        ),
        name="project",
    )(hidden_in, norm_gain.reshape(nt, feats), w_x, w_z, flat_bc, dt_rows)

    taps = conv_x.shape[0]
    conv_params = jnp.concatenate([conv_x, conv_bias_x[None]], axis=0)
    bc_params = jnp.concatenate([conv_bc, conv_bias_bc[None]], axis=0)
    bc_params = jnp.transpose(bc_params, (1, 0, 2))
    head_params = jnp.stack([dt_bias, decay_rate, skip_d]).reshape(3, ns, heads)
    head_params = jnp.pad(head_params, ((0, 0), (0, 0), (0, 128 - heads)))
    cols = feats
    return pl.pallas_call(
        functools.partial(mix_kernel, (ns, nt, heads)),
        out_shape=jax.ShapeDtypeStruct((rows, feats), jnp.bfloat16),
        in_specs=[vmem] * 7 + [anyw, vmem],
        out_specs=vmem,
        scratch_shapes=[
            pltpu.VMEM((8, width + bc_width), jnp.float32),
            pltpu.VMEM((heads, state_dim, head_dim), jnp.float32),
            pltpu.VMEM((ns, rows, width), jnp.bfloat16),
            pltpu.VMEM((ns, 8, rows), jnp.float32),
            pltpu.VMEM((ns, rows, width), jnp.bfloat16),
            pltpu.VMEM((ns, 8, rows), jnp.float32),
            pltpu.VMEM(w_out.shape, jnp.bfloat16),
            pltpu.VMEM((2, 2, rows, cols // 2), jnp.bfloat16),
            pltpu.VMEM((2, 2, rows, cols // 2), jnp.bfloat16),
            pltpu.VMEM((2, rows, cols // 2), jnp.bfloat16),
            pltpu.VMEM((2, rows, cols // 2), jnp.bfloat16),
            dma, dma((ns,)), dma((ns,)), dma((ns,)), dma((ns,)),
            dma((2, 2)), dma((2, 2)), dma((2,)), dma((2,)),
        ],
        compiler_params=pltpu.CompilerParams(
            collective_id=1, has_side_effects=True, vmem_limit_bytes=62 * 1024 * 1024
        ),
        name="mix",
    )(xz, bc, dt, conv_params, bc_params, head_params, out_gain[None], w_out, hidden_in)


def fits(mesh, args):
    ns, nt = mesh.shape["seq"], mesh.shape["tensor"]
    hidden_in, w_x, w_bc, decay_rate = args[0], args[2], args[4], args[7]
    if nt != 4 or ns % 2 or ns > 8:
        return False
    rows, feats = hidden_in.shape[0] // ns, hidden_in.shape[1] // nt
    groups, heads = w_bc.shape[1] // nt, decay_rate.shape[0] // nt
    if rows % SPAN or feats % 512 or heads % ns or ns % (2 * groups):
        return False
    width = w_x.shape[1] // (nt * ns)
    state = w_bc.shape[2] // 2
    return width % 256 == 0 and state == 128 and width * ns // heads == 128 and rows * hidden_in.shape[1] <= 384 * 4096


def solution(mesh):
    seq, tensor = mesh.shape["seq"], mesh.shape["tensor"]
    in_tail = (
        P("tensor"), P("tensor"), P(None, "tensor"), P(None, "tensor", None), P("tensor"), P("tensor", None),
        P("tensor"), P("tensor"), P("tensor", None),
    )

    def run(*args):
        if fits(mesh, args):
            return jax.shard_map(
                functools.partial(spread_heads, seq, tensor),
                mesh=mesh,
                in_specs=(
                    P("seq", "tensor"), P(), P("seq", "tensor"), P("seq", "tensor"),
                    P("seq", "tensor", None), P("seq", "tensor"),
                ) + in_tail,
                out_specs=P("seq", "tensor"),
                check_vma=False,
            )(*args)
        groups = args[4].shape[1] // tensor
        fold = 2 if groups % 2 == 0 and seq % 2 == 0 else 1
        split = Mesh(
            mesh.devices.reshape(seq // fold, fold, tensor), ("outer", "fold", "tensor")
        )
        both = ("outer", "fold")
        in_specs = (
            P(both, "tensor"), P(), P(both, "tensor"), P(both, "tensor"), P(both, "tensor", None), P(both, "tensor"),
        ) + in_tail
        return jax.shard_map(
            local, mesh=split, in_specs=in_specs, out_specs=P(both, "tensor"), check_vma=False
        )(*args)

    return run
```

```python
import functools

import jax
import jax.numpy as jnp
from jax import lax
from jax.experimental import pallas as pl
from jax.experimental.pallas import tpu as pltpu
from jax.sharding import Mesh, PartitionSpec as P

MESH = pl.DeviceIdType.MESH
SPAN = 128
RING_LIMIT = 8


epsilon = 1e-05


def rms_scale(values, norm_weight):
    return (
        values
        * lax.rsqrt(jnp.mean(values * values, axis=-1, keepdims=True) + epsilon)
        * norm_weight
    )


def causal_conv(padded, weight, bias_row):
    tap_count = weight.shape[0]
    out_length = padded.shape[0] - tap_count + 1
    running = bias_row
    for k in range(tap_count):
        running = running + weight[k] * padded[k : k + out_length].astype(jnp.float32)
    return jax.nn.silu(running).astype(jnp.bfloat16)


def span_terms(x_blocks, b_blocks, c_blocks, log_decay, dt_blocks):
    cum_decay = jnp.cumsum(log_decay, axis=1)
    scores = jnp.einsum("ctgn,csgn->cgts", c_blocks, b_blocks, preferred_element_type=jnp.float32)
    length = x_blocks.shape[1]
    causal_mask = lax.broadcasted_iota(jnp.int32, (length, length), 0) >= lax.broadcasted_iota(
        jnp.int32, (length, length), 1
    )
    cum_rows = jnp.transpose(cum_decay, (0, 2, 3, 1))
    decay_gap = cum_rows[..., :, None] - cum_rows[..., None, :]
    decay_mat = jnp.where(causal_mask, jnp.exp(jnp.where(causal_mask, decay_gap, 0.0)), 0.0)
    dt_cols = jnp.transpose(dt_blocks, (0, 2, 3, 1))[..., None, :]
    mix_weight = (scores[:, :, None] * decay_mat * dt_cols).astype(jnp.bfloat16)
    intra_out = jnp.einsum(
        "cgkts,csgkp->ctgkp", mix_weight, x_blocks, preferred_element_type=jnp.float32
    )
    tail_decay = jnp.exp(cum_decay[:, -1:] - cum_decay) * dt_blocks
    scaled = (x_blocks.astype(jnp.float32) * tail_decay[..., None]).astype(jnp.bfloat16)
    fresh_state = jnp.einsum(
        "csgkp,csgn->cgkpn", scaled, b_blocks, preferred_element_type=jnp.float32
    )
    return (cum_decay, intra_out, fresh_state)


def shifted(block, axis, distance):
    count = lax.axis_size(axis)
    return lax.ppermute(block, axis, [(i, (i + distance) % count) for i in range(count)])


def passed_along(block, axis, distance):
    devices = range(lax.axis_size(axis))
    return lax.ppermute(block, axis, [(i - distance, i) for i in devices if i - distance in devices])


def swapped(block, axis, bit):
    return lax.ppermute(block, axis, [(i, i ^ bit) for i in range(lax.axis_size(axis))])


def ring_pieces(own, axis):
    count = lax.axis_size(axis)
    pieces = [(0, 0, own)]
    ahead, behind = own, own
    for step in range(1, (count - 1) // 2 + 1):
        ahead, behind = shifted(ahead, axis, 1), shifted(behind, axis, -1)
        pieces += [(step, 0, ahead), (count - step, 0, behind)]
    if count % 2 == 0:
        half = own.shape[0] // 2
        pieces += [
            (count // 2, 0, shifted(ahead[:half], axis, 1)),
            (count // 2, half, shifted(behind[half:], axis, -1)),
        ]
    return pieces


def carried_in(total_log, state):
    count, mine = lax.axis_size("outer"), lax.axis_index("outer")
    logs, states = lax.all_gather((total_log, state), "outer")

    def hop(position, running):
        longer = jnp.exp(logs[position])[..., None, None] * running + states[position]
        return jnp.where(position < mine, longer, running)

    return lax.fori_loop(0, count - 1, hop, jnp.zeros_like(state))


def gather_tokens(hidden_in):
    tensor, fold = lax.axis_size("tensor"), lax.axis_size("fold")
    rows, cols = hidden_in.shape
    pieces = [(0, 0, hidden_in)]
    bits = []
    bit = tensor // 2
    while bit > 1:
        bits.append(("tensor", bit))
        bit //= 2
    if fold > 1:
        bits.append(("fold", 1))
    if tensor > 1:
        bits.append(("tensor", 1))
    for axis, bit in bits:
        pieces += [
            (j ^ bit, k, swapped(part, axis, bit)) if axis == "tensor" else (j, k ^ bit, swapped(part, axis, bit))
            for j, k, part in list(pieces)
        ]
    full = jnp.zeros((tensor, rows * fold, cols), hidden_in.dtype)
    me_t, me_f = lax.axis_index("tensor"), lax.axis_index("fold")
    for j, k, part in pieces:
        full = lax.dynamic_update_slice(full, part[None], (me_t ^ j, (me_f ^ k) * rows, 0))
    return full


def scatter_sum(partial, rows, cols):
    tensor, fold = lax.axis_size("tensor"), lax.axis_size("fold")
    me_t, me_f = lax.axis_index("tensor"), lax.axis_index("fold")
    if tensor > 1:
        pairs = partial.reshape(fold * rows, tensor // 2, 2, cols)
        core = me_t % 2
        keep = lax.dynamic_index_in_dim(pairs, core, 2, keepdims=False)
        send = lax.dynamic_index_in_dim(pairs, 1 - core, 2, keepdims=False)
        keep = keep.astype(jnp.float32) + swapped(send.astype(jnp.bfloat16), "tensor", 1).astype(jnp.float32)
    else:
        keep = partial.reshape(fold * rows, 1, cols).astype(jnp.float32)

    def over_fold(value):
        if fold == 1:
            return value
        split = value.reshape(fold, rows, *value.shape[1:])
        mine = lax.dynamic_index_in_dim(split, me_f, 0, keepdims=False)
        other = lax.dynamic_index_in_dim(split, 1 - me_f, 0, keepdims=False)
        return mine + swapped(other.astype(jnp.bfloat16), "fold", 1).astype(jnp.float32)

    def over_high(value):
        count = tensor // 2
        bit = tensor // 2
        while count > 1:
            split = value.reshape(value.shape[0], 2, count // 2, value.shape[-1])
            top = (me_t // bit) % 2
            mine = lax.dynamic_index_in_dim(split, top, 1, keepdims=False)
            other = lax.dynamic_index_in_dim(split, 1 - top, 1, keepdims=False)
            value = mine + swapped(other.astype(jnp.bfloat16), "tensor", bit).astype(jnp.float32)
            count, bit = count // 2, bit // 2
        return value

    half = cols // 2
    first = over_high(over_fold(keep[..., :half]))
    second = over_fold(over_high(keep[..., half:]))
    return jnp.concatenate([first.reshape(rows, half), second.reshape(rows, cols - half)], axis=1)


def local(
    hidden_in,
    norm_gain,
    w_x,
    w_z,
    w_bc,
    w_dt,
    dt_bias,
    decay_rate,
    conv_x,
    conv_bc,
    conv_bias_x,
    conv_bias_bc,
    skip_d,
    out_gain,
    w_out,
):
    fold = lax.axis_size("fold")
    me_f = lax.axis_index("fold")
    me_o = lax.axis_index("outer")
    outer = lax.axis_size("outer")

    def part(value, axis, which=None):
        size = value.shape[axis] // fold
        which = me_f if which is None else which
        return lax.dynamic_slice_in_dim(value, which * size, size, axis)

    depth = w_x.shape[0]
    groups = w_bc.shape[1] // fold
    bc_width = w_bc.shape[2]
    bc_flat = w_bc.reshape(depth, w_bc.shape[1] * bc_width)
    state_dim = bc_width // 2
    head_count = decay_rate.shape[0] // fold
    inner_width = w_x.shape[1] // fold
    head_dim = inner_width // head_count
    per_group = head_count // groups

    def weights(which):
        side = jnp.concatenate([part(bc_flat, 1, which), part(w_dt, 1, which)], axis=1)
        return [jnp.concatenate([part(w_x, 1, which), side], axis=1), part(w_z, 1, which)]

    own = weights(me_f)
    other = [swapped(block, "fold", 1) for block in weights(1 - me_f)] if fold > 1 else []
    gathered = gather_tokens(hidden_in)
    blocks, row_count, width = gathered.shape
    values = gathered.astype(jnp.float32)
    scale = lax.rsqrt(jnp.mean(values * values, axis=(0, 2), keepdims=True) + epsilon)
    normed = (values * scale * norm_gain.reshape(blocks, 1, width)).astype(jnp.bfloat16)
    per_block = max(width // depth, 1)
    if outer <= RING_LIMIT:
        normed = normed.reshape(blocks, row_count, per_block, width // per_block)
        normed = jnp.transpose(normed, (0, 2, 1, 3)).reshape(blocks * per_block, row_count, depth)
    else:
        normed = jnp.transpose(normed, (1, 0, 2)).reshape(row_count, blocks * width)
    rim_rows = conv_x.shape[0] - 1

    def projected(index):
        total = None
        if outer > RING_LIMIT:
            rows = lax.all_gather(own[index], "outer")
            if fold > 1:
                theirs = lax.all_gather(other[index], "outer")
                first, second = jnp.where(me_f == 0, rows, theirs), jnp.where(me_f == 0, theirs, rows)
                rows = jnp.stack([first, second], axis=1)
            rows = rows.reshape(normed.shape[1], own[index].shape[1])
            return jnp.dot(normed, rows, preferred_element_type=jnp.float32)
        for k, block in enumerate([own, other] if fold > 1 else [own]):
            for behind, offset, piece in ring_pieces(block[index], "outer"):
                owner = (me_o - behind + outer) % outer
                lhs = lax.dynamic_index_in_dim(normed, owner * fold + (me_f ^ k), 0, keepdims=False)
                lhs = lhs[:, offset : offset + piece.shape[0]]
                term = jnp.dot(lhs, piece, preferred_element_type=jnp.float32)
                total = term if total is None else total + term
        return total

    first = projected(0)
    proj_x = first[:, :inner_width].astype(jnp.bfloat16)
    side = first[:, inner_width:]
    dt_raw = side[:, groups * bc_width :]
    proj_bc = side[:, : groups * bc_width].astype(jnp.bfloat16)
    gate_z = projected(1).astype(jnp.bfloat16)
    edge_x, edge_bc = passed_along(
        (proj_x[row_count - rim_rows :], proj_bc[row_count - rim_rows :]), "outer", 1
    )
    padded_x = jnp.concatenate([edge_x, proj_x], axis=0)
    padded_bc = jnp.concatenate([edge_bc, proj_bc], axis=0)
    dt_vals = jax.nn.softplus(dt_raw + part(dt_bias, 0))
    x_conv = causal_conv(padded_x, part(conv_x, 1), part(conv_bias_x, 0))
    bc_conv = causal_conv(
        padded_bc,
        part(conv_bc, 1).reshape(conv_bc.shape[0], groups * bc_width),
        part(conv_bias_bc, 0).reshape(groups * bc_width),
    ).reshape(row_count, groups, bc_width)
    span_count = row_count // SPAN
    x_blocks = x_conv.reshape(span_count, SPAN, groups, per_group, head_dim)
    b_blocks = bc_conv[..., :state_dim].reshape(span_count, SPAN, groups, state_dim)
    c_blocks = bc_conv[..., state_dim:].reshape(span_count, SPAN, groups, state_dim)
    log_decay = (-dt_vals * part(decay_rate, 0)).reshape(span_count, SPAN, groups, per_group)
    dt_blocks = dt_vals.reshape(span_count, SPAN, groups, per_group)
    cum_decay, intra_out, fresh_state = span_terms(
        x_blocks, b_blocks, c_blocks, log_decay, dt_blocks
    )
    block_totals = cum_decay[:, -1]
    state = jnp.zeros((groups, per_group, head_dim, state_dim), jnp.float32)
    entering = []
    for i in range(span_count):
        entering.append(state)
        state = jnp.exp(block_totals[i])[..., None, None] * state + fresh_state[i]
    local_enter = jnp.stack(entering)
    before_log = jnp.cumsum(block_totals, axis=0) - block_totals
    total_log = jnp.sum(block_totals, axis=0)
    if outer > RING_LIMIT:
        incoming = carried_in(total_log, state)
    else:
        incoming = jnp.zeros_like(state)
        log_between = jnp.zeros_like(total_log)
        for distance in range(1, outer):
            arrived = passed_along(state, "outer", distance)
            incoming = incoming + jnp.exp(log_between)[..., None, None] * arrived
            log_between = log_between + passed_along(total_log, "outer", distance)
    enter_state = local_enter + jnp.exp(before_log)[..., None, None] * incoming[None]
    inter_out = jnp.exp(cum_decay)[..., None] * jnp.einsum(
        "ctgn,cgkpn->ctgkp", c_blocks, enter_state.astype(jnp.bfloat16), preferred_element_type=jnp.float32
    )
    skip_heads = part(skip_d, 0).reshape(groups, per_group)[..., None]
    ssm_out = (intra_out + inter_out + skip_heads * x_blocks.astype(jnp.float32)).reshape(
        row_count, inner_width
    )
    gated_out = ssm_out * jax.nn.silu(gate_z.astype(jnp.float32))
    grouped = gated_out.reshape(row_count, groups, inner_width // groups)
    normed_y = (
        rms_scale(grouped, part(out_gain, 0).reshape(groups, inner_width // groups))
        .reshape(row_count, inner_width)
        .astype(jnp.bfloat16)
    )
    partial = jnp.dot(normed_y, part(w_out, 0), preferred_element_type=jnp.float32)
    summed = scatter_sum(partial, *hidden_in.shape)
    return (hidden_in.astype(jnp.float32) + summed).astype(jnp.bfloat16)


def wait_in(dst, sem, me):
    pltpu.make_async_remote_copy(
        src_ref=dst, dst_ref=dst, send_sem=sem, recv_sem=sem, device_id=me, device_id_type=MESH
    ).wait_recv()


def wait_out(src, sem, me):
    pltpu.make_async_remote_copy(
        src_ref=src, dst_ref=src, send_sem=sem, recv_sem=sem, device_id=me, device_id_type=MESH
    ).wait_send()


def push(src, dst, send_sem, recv_sem, device):
    pltpu.make_async_remote_copy(
        src_ref=src, dst_ref=dst, send_sem=send_sem, recv_sem=recv_sem, device_id=device, device_id_type=MESH
    ).start()


def greet(partners):
    barrier = pltpu.get_barrier_semaphore()
    for device in partners:
        pl.semaphore_signal(barrier, inc=1, device_id=device, device_id_type=MESH)
    pl.semaphore_wait(barrier, len(partners))


def guarded(condition, action):
    if condition is None:
        action()
    else:
        pl.when(condition)(action)


def as_column(row):
    return jnp.transpose(jnp.broadcast_to(row[0:1], (row.shape[1], row.shape[1])))[:, 0:1]


def as_row(column):
    return jnp.transpose(jnp.broadcast_to(column, (column.shape[0], column.shape[0])))[0:8]


def layer_kernel(
    dims,
    x_ref, gain_ref, wx_ref, wz_ref, wbc_ref, wdt_ref,
    convx_ref, biasx_ref, convbc_ref, biasbc_ref, dt_bias_ref, decay_ref, skip_ref, out_gain_ref, wout_ref,
    out_ref,
    tok, wgt, side, acc, dtw, sums, rates, scales_in, bcs,
    tail, state, gated, norms, landed, norms_in, send_one, recv_one, send_two, recv_two, final,
    own_sem, tok_recv, z_up, z_down, x_send, y_send, core_send,
    w_send, w_recv, d_send, d_recv, s_send, s_recv, b_send, b_recv,
    r_send, r_recv, g_send, g_recv, n_send, n_recv, one_send, one_recv, two_send, two_recv,
):
    ns, nt, heads = dims
    nz = ns // 2
    rows, feats = x_ref.shape
    depth = wx_ref.shape[0]
    width = wx_ref.shape[1] // ns
    head_dim = width // heads
    lanes = 128
    s, t = lax.axis_index("seq"), lax.axis_index("tensor")
    z, x = s // 2, s % 2
    zz = nz - 1 - z
    y, core = t // 2, t % 2
    me = (s, t)
    sx = 2 * z + 1 - x
    ty = 2 * (1 - y) + core
    tc = 2 * y + 1 - core
    tyc = 2 * (1 - y) + 1 - core
    half_w = ns // 2
    near = z // (nz // 2)
    main = 2 * width
    groups = convbc_ref.shape[1]
    group_devices = ns // groups
    group_width = group_devices * width

    partners = [(lax.rem(s + i, ns), t) for i in range(1, ns)]
    partners += [(s, lax.rem(t + i, nt)) for i in range(1, nt)]
    greet(partners)

    def weight_parts(dest):
        group, half = dest // group_devices, dest % 2
        column = pl.multiple_of(dest * width, lanes)
        third = pl.multiple_of((group * 2 + half) * lanes, lanes)
        return [
            (wx_ref.at[:, pl.ds(column, width)], 0, width),
            (wz_ref.at[:, pl.ds(column, width)], width, width),
            (wbc_ref.at[:, pl.ds(third, lanes)], main, lanes),
        ]

    def send_weights(dest, which=(0, 1, 2)):
        parts = weight_parts(dest)
        for src, lane, size in [parts[i] for i in which]:
            push(src, wgt.at[s, :, pl.ds(lane, size)], w_send.at[dest], w_recv.at[s], (dest, t))

    pair = z + 1 - 2 * (z % 2)
    other = z - 1 + 2 * (z % 2)

    def across(flip):
        @pl.when((other >= 0) & (other < nz))
        def _():
            send_weights(2 * other + flip)

    def send_plane(plane):
        send_weights(2 * plane + x)
        send_weights(2 * plane + 1 - x)

    def send_weights_at(k):
        if k == 0:
            send_weights(2 * pair + x, (0, 1))
            send_weights(2 * pair + 1 - x)
            send_weights(sx)
            across(x)
        if k == 1:
            across(1 - x)
        if k >= 2:
            pl.when(z <= k - 2)(lambda: send_plane(k))
            pl.when(zz <= k - 2)(lambda: send_plane(nz - 1 - k))

    def inside(dz, action):
        if dz == 0:
            action()
        elif dz > 0:
            pl.when(z + dz < nz)(action)
        else:
            pl.when(z + dz >= 0)(action)

    own_copies = [
        pltpu.make_async_copy(src, wgt.at[s, :, pl.ds(lane, size)], own_sem.at[i])
        for i, (src, lane, size) in enumerate(weight_parts(s))
    ]
    send_weights(2 * pair + x, (2,))
    for copy in own_copies:
        copy.start()
    gain = gain_ref[:, pl.ds(pl.multiple_of(t * feats, lanes), feats)]

    def tok_at(si, ti):
        return tok.at[pl.ds(pl.multiple_of((si * nt + ti) * rows, lanes), rows), :]

    for r in range(0, rows, lanes):
        values = x_ref[r : r + lanes, :].astype(jnp.float32)
        sums[t, :, r : r + lanes] = as_row(jnp.sum(values * values, axis=1, keepdims=True))
        row = pl.multiple_of((s * nt + t) * rows + r, lanes)
        tok[pl.ds(row, lanes), :] = (values * gain).astype(jnp.bfloat16)
    dtw[s] = jnp.transpose(wdt_ref[...].astype(jnp.float32)).astype(jnp.bfloat16)

    def send_tok(si, ti, send_sem, device):
        push(tok_at(si, ti), tok_at(si, ti), send_sem, tok_recv.at[si, ti], device)

    def wait_tok(si, ti):
        wait_in(tok_at(si, ti), tok_recv.at[si, ti], me)

    def from_z(dz):
        zb = z + dz
        block = 2 * zb + x
        if dz != 0:
            wait_tok(block, t)
        if dz <= 0:
            pl.when(z < nz - 1)(lambda: send_tok(block, t, z_up.at[zb], (s + 2, t)))
        if dz >= 0:
            pl.when(z > 0)(lambda: send_tok(block, t, z_down.at[zb], (s - 2, t)))
        send_tok(block, t, x_send.at[zb], (sx, t))
        send_tok(block, t, y_send.at[block], (s, ty))
        send_tok(block, t, core_send.at[0, block], (s, tc))

    def from_x(dz):
        block = 2 * (z + dz) + 1 - x
        wait_tok(block, t)
        send_tok(block, t, y_send.at[block], (s, ty))
        send_tok(block, t, core_send.at[0, block], (s, tc))

    def from_y(dz):
        for flip in (x, 1 - x):
            block = 2 * (z + dz) + flip
            wait_tok(block, ty)
            send_tok(block, ty, core_send.at[1, block], (s, tc))

    def from_core(dz, which):
        for flip in (x, 1 - x):
            wait_tok(2 * (z + dz) + flip, which)

    steps = [0]
    for k in range(1, nz):
        steps += [-k, k]

    for i in range(1, nt):
        peer = lax.rem(t + i, nt)
        push(sums.at[t], sums.at[t], s_send.at[peer], s_recv.at[t], (s, peer))
    from_z(0)
    send_weights_at(0)
    for i in range(1, ns):
        dest = lax.rem(s + i, ns)
        push(dtw.at[s], dtw.at[s], d_send.at[dest], d_recv.at[s], (dest, t))

    def share_rates():
        for i in range(1, nt):
            peer = lax.rem(t + i, nt)
            wait_in(sums.at[peer], s_recv.at[peer], me)
        total = sums[0]
        for i in range(1, nt):
            total = total + sums[i]
        rates[s] = lax.rsqrt(total * (1.0 / (nt * feats)) + epsilon)
        for i in range(1, ns):
            dest = lax.rem(s + i, ns)
            push(rates.at[s], rates.at[s], r_send.at[dest], r_recv.at[s], (dest, t))

    from_x(0)
    for k in range(1, nz):
        for dz in (-k, k):
            inside(dz, lambda dz=dz: from_z(dz))
        send_weights_at(k)
        if k == 1:
            share_rates()
        if k > 1:
            for dz in (-(k - 1), k - 1):
                inside(dz, lambda dz=dz: from_x(dz))
        if k == 2:
            from_y(0)
    for dz in (-(nz - 1), nz - 1):
        inside(dz, lambda dz=dz: from_x(dz))
    for copy in own_copies:
        copy.wait()

    def weight_ready(source):
        @pl.when(source != s)
        def _():
            wait_in(wgt.at[source], w_recv.at[source], me)
            wait_in(dtw.at[source], d_recv.at[source], me)

        side[source, :, 0:lanes] = wgt[source, :, main:]
        short = dtw[source].astype(jnp.float32)
        short = pltpu.roll(short, lax.rem(short.shape[0] - s * heads, short.shape[0]), 0)
        padded = jnp.concatenate([short, jnp.zeros((lanes - short.shape[0], depth), jnp.float32)], axis=0)
        side[source, :, lanes:] = jnp.transpose(padded).astype(jnp.bfloat16)

    def product(block, part, tiles, put):
        first = part * (nt // 2)
        lhs = jnp.concatenate([tok_at(block, first + i)[...] for i in range(nt // 2)], axis=1)
        source = pl.ds(part * half_w, half_w)
        for n in tiles:
            if n < main:
                rhs = wgt[source, :, n : n + 256]
            else:
                rhs = side[source, :, n - main : n - main + 256]
            rhs = rhs.reshape(half_w * depth, 256)
            put(n, jnp.dot(lhs, rhs, preferred_element_type=jnp.float32))

    @pl.loop(0, half_w)
    def _(i):
        weight_ready(near * half_w + i)

    def begin(block):
        def put(n, value):
            acc[block, :, n : n + 256] = value

        product(block, near, range(0, main + 256, 256), put)

    for dz in steps:

        def group(dz=dz):
            if dz != 0:
                from_y(dz)
            from_core(dz, tc)
            from_core(dz, tyc)

            @pl.loop(0, 2)
            def _(flip):
                begin(2 * (z + dz) + flip)

        inside(dz, group)

    @pl.loop(0, half_w)
    def _(i):
        weight_ready((1 - near) * half_w + i)

    @pl.loop(0, ns)
    def _(block):
        @pl.when(block != s)
        def _():
            wait_in(rates.at[block], r_recv.at[block], me)

        for r in range(0, rows, lanes):
            row = rates[block, 0:1, r : r + lanes]
            scales_in[block, r : r + lanes, :] = jnp.transpose(jnp.broadcast_to(row, (lanes, lanes)))

    def scaled_sum(block, n, value):
        scale = scales_in[block]
        return (acc[block, :, n : n + 256] + value) * jnp.concatenate([scale, scale], axis=1)

    def first_part(block):
        def put(n, value):
            value = scaled_sum(block, n, value)
            bcs[x, block] = value[:, 0:lanes].astype(jnp.bfloat16)
            acc[block, :, main + lanes :] = value[:, lanes:]

        product(block, 1 - near, [main], put)
        push(bcs.at[x, block], bcs.at[x, block], b_send.at[block], b_recv.at[block], (sx, t))

    @pl.loop(0, ns)
    def _(block):
        first_part(block)

    def finish(block):
        def put(n, value):
            acc[block, :, n : n + 256] = scaled_sum(block, n, value)

        product(block, 1 - near, range(0, main, 256), put)

    tail[...] = jnp.zeros_like(tail)
    state[...] = jnp.zeros_like(state)
    column = pl.multiple_of(s * width, lanes)
    tap_count = convx_ref.shape[0]
    group = s // group_devices
    taps_x = [convx_ref[pl.ds(k, 1), pl.ds(column, width)] for k in range(tap_count)]
    taps_x.append(biasx_ref[:, pl.ds(column, width)])
    taps_bc = [convbc_ref[k, pl.ds(group, 1), :] for k in range(tap_count)]
    taps_bc.append(biasbc_ref[pl.ds(group, 1), :])
    head_lanes = lax.broadcasted_iota(jnp.int32, (1, lanes), 1)

    def lane_row(ref):
        row = jnp.zeros((1, lanes), jnp.float32)
        for h in range(heads):
            row = jnp.where(head_lanes == h, ref[s * heads + h], row)
        return row

    dt_bias, decay = lane_row(dt_bias_ref), lane_row(decay_ref)
    out_gain = out_gain_ref[:, pl.ds(column, width)]
    span_rows = lax.broadcasted_iota(jnp.int32, (SPAN, SPAN), 0)
    span_cols = lax.broadcasted_iota(jnp.int32, (SPAN, SPAN), 1)
    causal = span_rows >= span_cols
    lower = jnp.where(causal, 1.0, 0.0)

    def conv(previous, current, taps):
        padded = jnp.concatenate([previous, current], axis=0)
        running = taps[tap_count]
        for k in range(tap_count):
            start = 8 - (tap_count - 1) + k
            running = running + taps[k] * padded[start : start + SPAN]
        return (running * jax.nn.sigmoid(running)).astype(jnp.bfloat16)

    def rounded(block, r, first, size):
        return acc[block, r : r + SPAN, first : first + size].astype(jnp.bfloat16).astype(jnp.float32)

    def span(block, r):
        i = r // SPAN
        x_raw = rounded(block, r, 0, width)
        b_raw = bcs[0, block, r : r + SPAN, :].astype(jnp.float32)
        c_raw = bcs[1, block, r : r + SPAN, :].astype(jnp.float32)
        bc_raw = jnp.concatenate([b_raw, c_raw], axis=1)
        x_conv = conv(tail[:, 0:width], x_raw, taps_x)
        bc_conv = conv(tail[:, width:], bc_raw, taps_bc)
        tail[:, 0:width] = x_raw[SPAN - 8 :]
        tail[:, width:] = bc_raw[SPAN - 8 :]
        b_conv, c_conv = bc_conv[:, 0:lanes], bc_conv[:, lanes:]
        raw = acc[block, r : r + SPAN, main + lanes :] + dt_bias
        dt = jnp.maximum(raw, 0.0) + jnp.log1p(jnp.exp(-jnp.abs(raw)))
        cum = jnp.dot(lower, -dt * decay, precision=lax.Precision.HIGHEST, preferred_element_type=jnp.float32)
        cum_t = jnp.transpose(cum)
        dt_t = jnp.transpose(dt)
        scores = lax.dot_general(c_conv, b_conv, (((1,), (1,)), ((), ())), preferred_element_type=jnp.float32)
        b_t = jnp.transpose(b_conv.astype(jnp.float32)).astype(jnp.bfloat16)
        squares = None
        for h in range(heads):
            x_h = x_conv[:, h * head_dim : (h + 1) * head_dim]
            x_f = x_h.astype(jnp.float32)
            cum_h = cum[:, h : h + 1]
            gap = jnp.where(causal, cum_h - cum_t[h : h + 1, :], -jnp.inf)
            mix = (scores * jnp.exp(gap) * dt_t[h : h + 1, :]).astype(jnp.bfloat16)
            value = jnp.dot(mix, x_h, preferred_element_type=jnp.float32)
            last = cum[SPAN - 1 : SPAN, h : h + 1]
            scaled = (x_f * (jnp.exp(last - cum_h) * dt[:, h : h + 1])).astype(jnp.bfloat16)
            entering = state[h]
            value = value + jnp.exp(cum_h) * jnp.dot(
                c_conv, entering.astype(jnp.bfloat16), preferred_element_type=jnp.float32
            )
            state[h] = jnp.exp(last) * entering + jnp.dot(b_t, scaled, preferred_element_type=jnp.float32)
            value = value + skip_ref[s * heads + h] * x_f
            gate = rounded(block, r, width + h * head_dim, head_dim)
            value = value * (gate * jax.nn.sigmoid(gate))
            square = jnp.sum(value * value, axis=1, keepdims=True)
            squares = square if squares is None else squares + square
            gain = out_gain[:, h * head_dim : (h + 1) * head_dim]
            gated[i, block, :, h * head_dim : (h + 1) * head_dim] = (value * gain).astype(jnp.bfloat16)
        norms[i, block] = as_row(squares)

        @pl.when(block != s)
        def _():
            push(gated.at[i, block], landed.at[i, s], g_send.at[i, block], g_recv.at[i, s], (block, t))
            push(norms.at[i, block], norms_in.at[i, s], n_send.at[i, block], n_recv.at[i, s], (block, t))

        @pl.when(block == s)
        def _():
            landed[i, s] = gated[i, block]
            norms_in[i, s] = norms[i, block]

    def scan(block):
        wait_in(bcs.at[1 - x, block], b_recv.at[block], me)
        for r in range(0, rows, SPAN):
            span(block, r)

    @pl.loop(0, ns - 1)
    def _(block):
        finish(block)
        scan(block)

    finish(ns - 1)

    @pl.loop(0, ns)
    def _(block):
        wait_out(tok_at(block, t), y_send.at[block], me)
        wait_out(tok_at(block, t), core_send.at[0, block], me)
        wait_out(tok_at(block, t), core_send.at[1, block], me)

    for dz in steps:

        def drain(dz=dz):
            zb = z + dz
            if dz <= 0:
                pl.when(z < nz - 1)(lambda: wait_out(tok_at(0, 0), z_up.at[zb], me))
            if dz >= 0:
                pl.when(z > 0)(lambda: wait_out(tok_at(0, 0), z_down.at[zb], me))
            wait_out(tok_at(0, 0), x_send.at[zb], me)

        inside(dz, drain)

    inner = wout_ref.shape[0]
    def fetch(owner):
        return pltpu.make_async_copy(
            wout_ref.at[:, pl.ds(pl.multiple_of(owner * feats, lanes), feats)],
            tok.at[pl.ds(pl.multiple_of(owner * inner, lanes), inner), :],
            own_sem.at[owner],
        )

    for owner in (tyc, ty, tc, t):
        fetch(owner).start()
    scan(ns - 1)

    @pl.loop(0, rows // SPAN)
    def _(r):
        for i in range(1, ns):
            source = lax.rem(s + i, ns)
            wait_in(landed.at[r, source], g_recv.at[r, source], me)
            wait_in(norms_in.at[r, source], n_recv.at[r, source], me)
        scales, lhs = [], []
        for g in range(groups):
            total = norms_in[r, g * group_devices]
            for i in range(1, group_devices):
                total = total + norms_in[r, g * group_devices + i]
            scales.append(as_column(lax.rsqrt(total * (1.0 / group_width) + epsilon)))
            lhs.append(jnp.concatenate([landed[r, g * group_devices + i] for i in range(group_devices)], axis=1))

        def partial(owner):
            @pl.when(r == 0)
            def _():
                fetch(owner).wait()

            total = None
            for g in range(groups):
                row = pl.multiple_of(owner * inner + g * group_width, lanes)
                term = scales[g] * jnp.dot(lhs[g], tok[pl.ds(row, group_width), :], preferred_element_type=jnp.float32)
                total = term if total is None else total + term
            return total

        def to_core(slot, owner):
            send_one[r, slot] = partial(owner).astype(jnp.bfloat16)
            push(send_one.at[r, slot], recv_one.at[r, slot], one_send.at[r, slot], one_recv.at[r, slot], (s, tc))

        to_core(0, tyc)
        mine = partial(ty)
        wait_in(recv_one.at[r, 0], one_recv.at[r, 0], me)
        send_two[r] = (mine + recv_one[r, 0].astype(jnp.float32)).astype(jnp.bfloat16)
        push(send_two.at[r], recv_two.at[r], two_send.at[r], two_recv.at[r], (s, ty))
        to_core(1, tc)
        mine = partial(t)
        wait_in(recv_one.at[r, 1], one_recv.at[r, 1], me)
        span = pl.ds(pl.multiple_of(r * SPAN, SPAN), SPAN)
        final[r] = mine + recv_one[r, 1].astype(jnp.float32) + x_ref[span, :].astype(jnp.float32)

    for r in range(rows // SPAN):
        wait_in(recv_two.at[r], two_recv.at[r], me)
        out_ref[r * SPAN : (r + 1) * SPAN, :] = (final[r] + recv_two[r].astype(jnp.float32)).astype(jnp.bfloat16)

    for i in range(1, ns):
        dest = lax.rem(s + i, ns)
        for r in range(rows // SPAN):
            wait_out(gated.at[r, dest], g_send.at[r, dest], me)
            wait_out(norms.at[r, dest], n_send.at[r, dest], me)
        wait_out(wgt.at[dest], w_send.at[dest], me)
        wait_out(dtw.at[dest], d_send.at[dest], me)
        wait_out(rates.at[dest], r_send.at[dest], me)

    @pl.loop(0, ns)
    def _(block):
        wait_out(bcs.at[x, block], b_send.at[block], me)

    for i in range(1, nt):
        wait_out(sums.at[t], s_send.at[lax.rem(t + i, nt)], me)
    for r in range(rows // SPAN):
        for slot in range(2):
            wait_out(send_one.at[r, slot], one_send.at[r, slot], me)
        wait_out(send_two.at[r], two_send.at[r], me)


def spread_heads(ns, nt, *args):
    (hidden_in, norm_gain, w_x, w_z, w_bc, w_dt, dt_bias, decay_rate,
     conv_x, conv_bc, conv_bias_x, conv_bias_bc, skip_d, out_gain, w_out) = args
    rows, feats = hidden_in.shape
    depth, columns = w_x.shape
    width = columns // ns
    heads = decay_rate.shape[0] // ns
    groups, bc_width = w_bc.shape[1], w_bc.shape[2]
    state_dim = bc_width // 2
    head_dim = width // heads
    flat_bc = w_bc.reshape(depth, groups * bc_width)
    hbm = pl.BlockSpec(memory_space=pl.ANY)
    vmem = pl.BlockSpec(memory_space=pltpu.VMEM)
    smem = pl.BlockSpec(memory_space=pltpu.SMEM)
    dma = pltpu.SemaphoreType.DMA
    spans = rows // SPAN
    return pl.pallas_call(
        functools.partial(layer_kernel, (ns, nt, heads)),
        out_shape=jax.ShapeDtypeStruct((rows, feats), jnp.bfloat16),
        in_specs=[vmem, vmem, hbm, hbm, hbm, vmem, vmem, vmem, vmem, vmem, smem, smem, smem, vmem, hbm],
        out_specs=vmem,
        scratch_shapes=[
            pltpu.VMEM((ns * nt * rows, feats), jnp.bfloat16),
            pltpu.VMEM((ns, depth, 2 * width + 128), jnp.bfloat16),
            pltpu.VMEM((ns, depth, 256), jnp.bfloat16),
            pltpu.VMEM((ns, rows, 2 * width + 256), jnp.float32),
            pltpu.VMEM((ns, w_dt.shape[1], depth), jnp.bfloat16),
            pltpu.VMEM((nt, 8, rows), jnp.float32),
            pltpu.VMEM((ns, 8, rows), jnp.float32),
            pltpu.VMEM((ns, rows, 128), jnp.float32),
            pltpu.VMEM((2, ns, rows, 128), jnp.bfloat16),
            pltpu.VMEM((8, width + bc_width), jnp.float32),
            pltpu.VMEM((heads, state_dim, head_dim), jnp.float32),
            pltpu.VMEM((spans, ns, SPAN, width), jnp.bfloat16),
            pltpu.VMEM((spans, ns, 8, SPAN), jnp.float32),
            pltpu.VMEM((spans, ns, SPAN, width), jnp.bfloat16),
            pltpu.VMEM((spans, ns, 8, SPAN), jnp.float32),
            pltpu.VMEM((spans, 2, SPAN, feats), jnp.bfloat16),
            pltpu.VMEM((spans, 2, SPAN, feats), jnp.bfloat16),
            pltpu.VMEM((spans, SPAN, feats), jnp.bfloat16),
            pltpu.VMEM((spans, SPAN, feats), jnp.bfloat16),
            pltpu.VMEM((spans, SPAN, feats), jnp.float32),
            dma((4,)), dma((ns, nt)), dma((ns // 2,)), dma((ns // 2,)), dma((ns // 2,)), dma((ns,)), dma((2, ns)),
            dma((ns,)), dma((ns,)), dma((ns,)), dma((ns,)), dma((nt,)), dma((nt,)), dma((ns,)), dma((ns,)),
            dma((ns,)), dma((ns,)),
            dma((spans, ns)), dma((spans, ns)), dma((spans, ns)), dma((spans, ns)),
            dma((spans, 2)), dma((spans, 2)), dma((spans,)), dma((spans,)),
        ],
        compiler_params=pltpu.CompilerParams(
            collective_id=0, has_side_effects=True, vmem_limit_bytes=63 * 1024 * 1024
        ),
        name="layer",
    )(
        hidden_in, norm_gain.reshape(1, nt * feats), w_x, w_z, flat_bc, w_dt,
        conv_x, conv_bias_x.reshape(1, columns), conv_bc, conv_bias_bc, dt_bias, decay_rate, skip_d,
        out_gain.reshape(1, columns), w_out,
    )


def fits(mesh, args):
    ns, nt = mesh.shape["seq"], mesh.shape["tensor"]
    hidden_in, w_x, w_bc, decay_rate = args[0], args[2], args[4], args[7]
    if nt != 4 or ns % 2 or ns > 8:
        return False
    rows, feats = hidden_in.shape[0] // ns, hidden_in.shape[1] // nt
    groups, heads = w_bc.shape[1] // nt, decay_rate.shape[0] // nt
    if rows % SPAN or feats % 512 or heads % ns or ns % (2 * groups) or ns % 4 or (decay_rate.shape[0] // nt) % 16:
        return False
    width = w_x.shape[1] // (nt * ns)
    state = w_bc.shape[2] // 2
    if args[14].shape[0] // nt > hidden_in.shape[0]:
        return False
    return width % 256 == 0 and state == 128 and width * ns // heads == 128 and rows * hidden_in.shape[1] <= 384 * 4096


def solution(mesh):
    seq, tensor = mesh.shape["seq"], mesh.shape["tensor"]
    in_tail = (
        P("tensor"), P("tensor"), P(None, "tensor"), P(None, "tensor", None), P("tensor"), P("tensor", None),
        P("tensor"), P("tensor"), P("tensor", None),
    )

    def run(*args):
        if fits(mesh, args):
            return jax.shard_map(
                functools.partial(spread_heads, seq, tensor),
                mesh=mesh,
                in_specs=(
                    P("seq", "tensor"), P(), P("seq", "tensor"), P("seq", "tensor"),
                    P("seq", "tensor", None), P("seq", "tensor"),
                ) + in_tail,
                out_specs=P("seq", "tensor"),
                check_vma=False,
            )(*args)
        groups = args[4].shape[1] // tensor
        fold = 2 if groups % 2 == 0 and seq % 2 == 0 else 1
        split = Mesh(
            mesh.devices.reshape(seq // fold, fold, tensor), ("outer", "fold", "tensor")
        )
        both = ("outer", "fold")
        in_specs = (
            P(both, "tensor"), P(), P(both, "tensor"), P(both, "tensor"), P(both, "tensor", None), P(both, "tensor"),
        ) + in_tail
        return jax.shard_map(
            local, mesh=split, in_specs=in_specs, out_specs=P(both, "tensor"), check_vma=False
        )(*args)

    return run
```

```python
import functools

import jax
import jax.numpy as jnp
from jax import lax
from jax.experimental import pallas as pl
from jax.experimental.pallas import tpu as pltpu
from jax.sharding import Mesh, PartitionSpec as P

MESH = pl.DeviceIdType.MESH
SPAN = 128
RING_LIMIT = 8


epsilon = 1e-05


def rms_scale(values, norm_weight):
    return (
        values
        * lax.rsqrt(jnp.mean(values * values, axis=-1, keepdims=True) + epsilon)
        * norm_weight
    )


def causal_conv(padded, weight, bias_row):
    tap_count = weight.shape[0]
    out_length = padded.shape[0] - tap_count + 1
    running = bias_row
    for k in range(tap_count):
        running = running + weight[k] * padded[k : k + out_length].astype(jnp.float32)
    return jax.nn.silu(running).astype(jnp.bfloat16)


def span_terms(x_blocks, b_blocks, c_blocks, log_decay, dt_blocks):
    cum_decay = jnp.cumsum(log_decay, axis=1)
    scores = jnp.einsum("ctgn,csgn->cgts", c_blocks, b_blocks, preferred_element_type=jnp.float32)
    length = x_blocks.shape[1]
    causal_mask = lax.broadcasted_iota(jnp.int32, (length, length), 0) >= lax.broadcasted_iota(
        jnp.int32, (length, length), 1
    )
    cum_rows = jnp.transpose(cum_decay, (0, 2, 3, 1))
    decay_gap = cum_rows[..., :, None] - cum_rows[..., None, :]
    decay_mat = jnp.where(causal_mask, jnp.exp(jnp.where(causal_mask, decay_gap, 0.0)), 0.0)
    dt_cols = jnp.transpose(dt_blocks, (0, 2, 3, 1))[..., None, :]
    mix_weight = (scores[:, :, None] * decay_mat * dt_cols).astype(jnp.bfloat16)
    intra_out = jnp.einsum(
        "cgkts,csgkp->ctgkp", mix_weight, x_blocks, preferred_element_type=jnp.float32
    )
    tail_decay = jnp.exp(cum_decay[:, -1:] - cum_decay) * dt_blocks
    scaled = (x_blocks.astype(jnp.float32) * tail_decay[..., None]).astype(jnp.bfloat16)
    fresh_state = jnp.einsum(
        "csgkp,csgn->cgkpn", scaled, b_blocks, preferred_element_type=jnp.float32
    )
    return (cum_decay, intra_out, fresh_state)


def shifted(block, axis, distance):
    count = lax.axis_size(axis)
    return lax.ppermute(block, axis, [(i, (i + distance) % count) for i in range(count)])


def passed_along(block, axis, distance):
    devices = range(lax.axis_size(axis))
    return lax.ppermute(block, axis, [(i - distance, i) for i in devices if i - distance in devices])


def swapped(block, axis, bit):
    return lax.ppermute(block, axis, [(i, i ^ bit) for i in range(lax.axis_size(axis))])


def ring_pieces(own, axis):
    count = lax.axis_size(axis)
    pieces = [(0, 0, own)]
    ahead, behind = own, own
    for step in range(1, (count - 1) // 2 + 1):
        ahead, behind = shifted(ahead, axis, 1), shifted(behind, axis, -1)
        pieces += [(step, 0, ahead), (count - step, 0, behind)]
    if count % 2 == 0:
        half = own.shape[0] // 2
        pieces += [
            (count // 2, 0, shifted(ahead[:half], axis, 1)),
            (count // 2, half, shifted(behind[half:], axis, -1)),
        ]
    return pieces


def carried_in(total_log, state):
    count, mine = lax.axis_size("outer"), lax.axis_index("outer")
    logs, states = lax.all_gather((total_log, state), "outer")

    def hop(position, running):
        longer = jnp.exp(logs[position])[..., None, None] * running + states[position]
        return jnp.where(position < mine, longer, running)

    return lax.fori_loop(0, count - 1, hop, jnp.zeros_like(state))


def gather_tokens(hidden_in):
    tensor, fold = lax.axis_size("tensor"), lax.axis_size("fold")
    rows, cols = hidden_in.shape
    pieces = [(0, 0, hidden_in)]
    bits = []
    bit = tensor // 2
    while bit > 1:
        bits.append(("tensor", bit))
        bit //= 2
    if fold > 1:
        bits.append(("fold", 1))
    if tensor > 1:
        bits.append(("tensor", 1))
    for axis, bit in bits:
        pieces += [
            (j ^ bit, k, swapped(part, axis, bit)) if axis == "tensor" else (j, k ^ bit, swapped(part, axis, bit))
            for j, k, part in list(pieces)
        ]
    full = jnp.zeros((tensor, rows * fold, cols), hidden_in.dtype)
    me_t, me_f = lax.axis_index("tensor"), lax.axis_index("fold")
    for j, k, part in pieces:
        full = lax.dynamic_update_slice(full, part[None], (me_t ^ j, (me_f ^ k) * rows, 0))
    return full


def scatter_sum(partial, rows, cols):
    tensor, fold = lax.axis_size("tensor"), lax.axis_size("fold")
    me_t, me_f = lax.axis_index("tensor"), lax.axis_index("fold")
    if tensor > 1:
        pairs = partial.reshape(fold * rows, tensor // 2, 2, cols)
        core = me_t % 2
        keep = lax.dynamic_index_in_dim(pairs, core, 2, keepdims=False)
        send = lax.dynamic_index_in_dim(pairs, 1 - core, 2, keepdims=False)
        keep = keep.astype(jnp.float32) + swapped(send.astype(jnp.bfloat16), "tensor", 1).astype(jnp.float32)
    else:
        keep = partial.reshape(fold * rows, 1, cols).astype(jnp.float32)

    def over_fold(value):
        if fold == 1:
            return value
        split = value.reshape(fold, rows, *value.shape[1:])
        mine = lax.dynamic_index_in_dim(split, me_f, 0, keepdims=False)
        other = lax.dynamic_index_in_dim(split, 1 - me_f, 0, keepdims=False)
        return mine + swapped(other.astype(jnp.bfloat16), "fold", 1).astype(jnp.float32)

    def over_high(value):
        count = tensor // 2
        bit = tensor // 2
        while count > 1:
            split = value.reshape(value.shape[0], 2, count // 2, value.shape[-1])
            top = (me_t // bit) % 2
            mine = lax.dynamic_index_in_dim(split, top, 1, keepdims=False)
            other = lax.dynamic_index_in_dim(split, 1 - top, 1, keepdims=False)
            value = mine + swapped(other.astype(jnp.bfloat16), "tensor", bit).astype(jnp.float32)
            count, bit = count // 2, bit // 2
        return value

    half = cols // 2
    first = over_high(over_fold(keep[..., :half]))
    second = over_fold(over_high(keep[..., half:]))
    return jnp.concatenate([first.reshape(rows, half), second.reshape(rows, cols - half)], axis=1)


def local(
    hidden_in,
    norm_gain,
    w_x,
    w_z,
    w_bc,
    w_dt,
    dt_bias,
    decay_rate,
    conv_x,
    conv_bc,
    conv_bias_x,
    conv_bias_bc,
    skip_d,
    out_gain,
    w_out,
):
    fold = lax.axis_size("fold")
    me_f = lax.axis_index("fold")
    me_o = lax.axis_index("outer")
    outer = lax.axis_size("outer")

    def part(value, axis, which=None):
        size = value.shape[axis] // fold
        which = me_f if which is None else which
        return lax.dynamic_slice_in_dim(value, which * size, size, axis)

    depth = w_x.shape[0]
    groups = w_bc.shape[1] // fold
    bc_width = w_bc.shape[2]
    bc_flat = w_bc.reshape(depth, w_bc.shape[1] * bc_width)
    state_dim = bc_width // 2
    head_count = decay_rate.shape[0] // fold
    inner_width = w_x.shape[1] // fold
    head_dim = inner_width // head_count
    per_group = head_count // groups

    def weights(which):
        side = jnp.concatenate([part(bc_flat, 1, which), part(w_dt, 1, which)], axis=1)
        return [jnp.concatenate([part(w_x, 1, which), side], axis=1), part(w_z, 1, which)]

    own = weights(me_f)
    other = [swapped(block, "fold", 1) for block in weights(1 - me_f)] if fold > 1 else []
    gathered = gather_tokens(hidden_in)
    blocks, row_count, width = gathered.shape
    values = gathered.astype(jnp.float32)
    scale = lax.rsqrt(jnp.mean(values * values, axis=(0, 2), keepdims=True) + epsilon)
    normed = (values * scale * norm_gain.reshape(blocks, 1, width)).astype(jnp.bfloat16)
    per_block = max(width // depth, 1)
    if outer <= RING_LIMIT:
        normed = normed.reshape(blocks, row_count, per_block, width // per_block)
        normed = jnp.transpose(normed, (0, 2, 1, 3)).reshape(blocks * per_block, row_count, depth)
    else:
        normed = jnp.transpose(normed, (1, 0, 2)).reshape(row_count, blocks * width)
    rim_rows = conv_x.shape[0] - 1

    def projected(index):
        total = None
        if outer > RING_LIMIT:
            rows = lax.all_gather(own[index], "outer")
            if fold > 1:
                theirs = lax.all_gather(other[index], "outer")
                first, second = jnp.where(me_f == 0, rows, theirs), jnp.where(me_f == 0, theirs, rows)
                rows = jnp.stack([first, second], axis=1)
            rows = rows.reshape(normed.shape[1], own[index].shape[1])
            return jnp.dot(normed, rows, preferred_element_type=jnp.float32)
        for k, block in enumerate([own, other] if fold > 1 else [own]):
            for behind, offset, piece in ring_pieces(block[index], "outer"):
                owner = (me_o - behind + outer) % outer
                lhs = lax.dynamic_index_in_dim(normed, owner * fold + (me_f ^ k), 0, keepdims=False)
                lhs = lhs[:, offset : offset + piece.shape[0]]
                term = jnp.dot(lhs, piece, preferred_element_type=jnp.float32)
                total = term if total is None else total + term
        return total

    first = projected(0)
    proj_x = first[:, :inner_width].astype(jnp.bfloat16)
    side = first[:, inner_width:]
    dt_raw = side[:, groups * bc_width :]
    proj_bc = side[:, : groups * bc_width].astype(jnp.bfloat16)
    gate_z = projected(1).astype(jnp.bfloat16)
    edge_x, edge_bc = passed_along(
        (proj_x[row_count - rim_rows :], proj_bc[row_count - rim_rows :]), "outer", 1
    )
    padded_x = jnp.concatenate([edge_x, proj_x], axis=0)
    padded_bc = jnp.concatenate([edge_bc, proj_bc], axis=0)
    dt_vals = jax.nn.softplus(dt_raw + part(dt_bias, 0))
    x_conv = causal_conv(padded_x, part(conv_x, 1), part(conv_bias_x, 0))
    bc_conv = causal_conv(
        padded_bc,
        part(conv_bc, 1).reshape(conv_bc.shape[0], groups * bc_width),
        part(conv_bias_bc, 0).reshape(groups * bc_width),
    ).reshape(row_count, groups, bc_width)
    span_count = row_count // SPAN
    x_blocks = x_conv.reshape(span_count, SPAN, groups, per_group, head_dim)
    b_blocks = bc_conv[..., :state_dim].reshape(span_count, SPAN, groups, state_dim)
    c_blocks = bc_conv[..., state_dim:].reshape(span_count, SPAN, groups, state_dim)
    log_decay = (-dt_vals * part(decay_rate, 0)).reshape(span_count, SPAN, groups, per_group)
    dt_blocks = dt_vals.reshape(span_count, SPAN, groups, per_group)
    cum_decay, intra_out, fresh_state = span_terms(
        x_blocks, b_blocks, c_blocks, log_decay, dt_blocks
    )
    block_totals = cum_decay[:, -1]
    state = jnp.zeros((groups, per_group, head_dim, state_dim), jnp.float32)
    entering = []
    for i in range(span_count):
        entering.append(state)
        state = jnp.exp(block_totals[i])[..., None, None] * state + fresh_state[i]
    local_enter = jnp.stack(entering)
    before_log = jnp.cumsum(block_totals, axis=0) - block_totals
    total_log = jnp.sum(block_totals, axis=0)
    if outer > RING_LIMIT:
        incoming = carried_in(total_log, state)
    else:
        incoming = jnp.zeros_like(state)
        log_between = jnp.zeros_like(total_log)
        for distance in range(1, outer):
            arrived = passed_along(state, "outer", distance)
            incoming = incoming + jnp.exp(log_between)[..., None, None] * arrived
            log_between = log_between + passed_along(total_log, "outer", distance)
    enter_state = local_enter + jnp.exp(before_log)[..., None, None] * incoming[None]
    inter_out = jnp.exp(cum_decay)[..., None] * jnp.einsum(
        "ctgn,cgkpn->ctgkp", c_blocks, enter_state.astype(jnp.bfloat16), preferred_element_type=jnp.float32
    )
    skip_heads = part(skip_d, 0).reshape(groups, per_group)[..., None]
    ssm_out = (intra_out + inter_out + skip_heads * x_blocks.astype(jnp.float32)).reshape(
        row_count, inner_width
    )
    gated_out = ssm_out * jax.nn.silu(gate_z.astype(jnp.float32))
    grouped = gated_out.reshape(row_count, groups, inner_width // groups)
    normed_y = (
        rms_scale(grouped, part(out_gain, 0).reshape(groups, inner_width // groups))
        .reshape(row_count, inner_width)
        .astype(jnp.bfloat16)
    )
    partial = jnp.dot(normed_y, part(w_out, 0), preferred_element_type=jnp.float32)
    summed = scatter_sum(partial, *hidden_in.shape)
    return (hidden_in.astype(jnp.float32) + summed).astype(jnp.bfloat16)


def wait_in(dst, sem, me):
    pltpu.make_async_remote_copy(
        src_ref=dst, dst_ref=dst, send_sem=sem, recv_sem=sem, device_id=me, device_id_type=MESH
    ).wait_recv()


def wait_out(src, sem, me):
    pltpu.make_async_remote_copy(
        src_ref=src, dst_ref=src, send_sem=sem, recv_sem=sem, device_id=me, device_id_type=MESH
    ).wait_send()


def push(src, dst, send_sem, recv_sem, device):
    pltpu.make_async_remote_copy(
        src_ref=src, dst_ref=dst, send_sem=send_sem, recv_sem=recv_sem, device_id=device, device_id_type=MESH
    ).start()


def greet(partners):
    barrier = pltpu.get_barrier_semaphore()
    for device in partners:
        pl.semaphore_signal(barrier, inc=1, device_id=device, device_id_type=MESH)
    pl.semaphore_wait(barrier, len(partners))


def guarded(condition, action):
    if condition is None:
        action()
    else:
        pl.when(condition)(action)


def as_column(row):
    return jnp.transpose(jnp.broadcast_to(row[0:1], (row.shape[1], row.shape[1])))[:, 0:1]


def as_row(column):
    return jnp.transpose(jnp.broadcast_to(column, (column.shape[0], column.shape[0])))[0:8]


def layer_kernel(
    dims,
    x_ref, gain_ref, wx_ref, wz_ref, wbc_ref, wdt_ref,
    convx_ref, biasx_ref, convbc_ref, biasbc_ref, dt_bias_ref, decay_ref, skip_ref, out_gain_ref, wout_ref,
    out_ref,
    tok, wgt, side, acc, dtw, sums, rates, scales_in, bcs,
    tail, state, gated, norms, landed, norms_in, send_one, recv_one, send_two, recv_two, final,
    own_sem, tok_recv, z_up, z_down, x_send, y_send, core_send,
    w_send, w_recv, d_send, d_recv, s_send, s_recv, b_send, b_recv,
    r_send, r_recv, g_send, g_recv, n_send, n_recv, one_send, one_recv, two_send, two_recv,
):
    ns, nt, heads = dims
    nz = ns // 2
    rows, feats = x_ref.shape
    depth = wx_ref.shape[0]
    width = wx_ref.shape[1] // ns
    head_dim = width // heads
    lanes = 128
    s, t = lax.axis_index("seq"), lax.axis_index("tensor")
    z, x = s // 2, s % 2
    zz = nz - 1 - z
    y, core = t // 2, t % 2
    me = (s, t)
    sx = 2 * z + 1 - x
    ty = 2 * (1 - y) + core
    tc = 2 * y + 1 - core
    tyc = 2 * (1 - y) + 1 - core
    half_w = ns // 2
    near = z // (nz // 2)
    main = 2 * width
    groups = convbc_ref.shape[1]
    group_devices = ns // groups
    group_width = group_devices * width

    partners = [(lax.rem(s + i, ns), t) for i in range(1, ns)]
    partners += [(s, lax.rem(t + i, nt)) for i in range(1, nt)]
    greet(partners)

    def weight_parts(dest):
        group, half = dest // group_devices, dest % 2
        column = pl.multiple_of(dest * width, lanes)
        third = pl.multiple_of((group * 2 + half) * lanes, lanes)
        return [
            (wx_ref.at[:, pl.ds(column, width)], 0, width),
            (wz_ref.at[:, pl.ds(column, width)], width, width),
            (wbc_ref.at[:, pl.ds(third, lanes)], main, lanes),
        ]

    def send_weights(dest, which=(0, 1, 2)):
        parts = weight_parts(dest)
        for src, lane, size in [parts[i] for i in which]:
            push(src, wgt.at[s, :, pl.ds(lane, size)], w_send.at[dest], w_recv.at[s], (dest, t))

    pair = z + 1 - 2 * (z % 2)
    other = z - 1 + 2 * (z % 2)

    def across(flip):
        @pl.when((other >= 0) & (other < nz))
        def _():
            send_weights(2 * other + flip)

    def send_plane(plane):
        send_weights(2 * plane + x)
        send_weights(2 * plane + 1 - x)

    def send_weights_at(k):
        if k == 0:
            send_weights(sx)
        if k == 1:
            send_weights(2 * pair + x, (0, 1))
            send_weights(2 * pair + 1 - x)
            across(x)
            across(1 - x)
        if k >= 2:
            pl.when(z == 0)(lambda: send_plane(k))
            pl.when(zz == 0)(lambda: send_plane(nz - 1 - k))
            if k + 1 < nz:
                pl.when((z >= 1) & (z <= k - 1))(lambda: send_plane(k + 1))
                pl.when((zz >= 1) & (zz <= k - 1))(lambda: send_plane(nz - 2 - k))

    def inside(dz, action):
        if dz == 0:
            action()
        elif dz > 0:
            pl.when(z + dz < nz)(action)
        else:
            pl.when(z + dz >= 0)(action)

    own_copies = [
        pltpu.make_async_copy(src, wgt.at[s, :, pl.ds(lane, size)], own_sem.at[i])
        for i, (src, lane, size) in enumerate(weight_parts(s))
    ]
    send_weights(2 * pair + x, (2,))
    for copy in own_copies:
        copy.start()
    gain = gain_ref[:, pl.ds(pl.multiple_of(t * feats, lanes), feats)]

    def tok_at(si, ti):
        return tok.at[pl.ds(pl.multiple_of((si * nt + ti) * rows, lanes), rows), :]

    for r in range(0, rows, lanes):
        values = x_ref[r : r + lanes, :].astype(jnp.float32)
        sums[t, :, r : r + lanes] = as_row(jnp.sum(values * values, axis=1, keepdims=True))
        row = pl.multiple_of((s * nt + t) * rows + r, lanes)
        tok[pl.ds(row, lanes), :] = (values * gain).astype(jnp.bfloat16)
    dtw[s] = jnp.transpose(wdt_ref[...].astype(jnp.float32)).astype(jnp.bfloat16)

    def send_tok(si, ti, send_sem, device):
        push(tok_at(si, ti), tok_at(si, ti), send_sem, tok_recv.at[si, ti], device)

    def wait_tok(si, ti):
        wait_in(tok_at(si, ti), tok_recv.at[si, ti], me)

    def from_z(dz):
        zb = z + dz
        block = 2 * zb + x
        if dz != 0:
            wait_tok(block, t)
        if dz <= 0:
            pl.when(z < nz - 1)(lambda: send_tok(block, t, z_up.at[zb], (s + 2, t)))
        if dz >= 0:
            pl.when(z > 0)(lambda: send_tok(block, t, z_down.at[zb], (s - 2, t)))
        send_tok(block, t, x_send.at[zb], (sx, t))
        send_tok(block, t, y_send.at[block], (s, ty))
        send_tok(block, t, core_send.at[0, block], (s, tc))

    def from_x(dz):
        block = 2 * (z + dz) + 1 - x
        wait_tok(block, t)
        send_tok(block, t, y_send.at[block], (s, ty))
        send_tok(block, t, core_send.at[0, block], (s, tc))

    def from_y(dz):
        for flip in (x, 1 - x):
            block = 2 * (z + dz) + flip
            wait_tok(block, ty)
            send_tok(block, ty, core_send.at[1, block], (s, tc))

    def from_core(dz, which):
        for flip in (x, 1 - x):
            wait_tok(2 * (z + dz) + flip, which)

    steps = [0]
    for k in range(1, nz):
        steps += [-k, k]

    for i in range(1, nt):
        peer = lax.rem(t + i, nt)
        push(sums.at[t], sums.at[t], s_send.at[peer], s_recv.at[t], (s, peer))
    from_z(0)
    send_weights_at(0)
    for i in range(1, ns):
        dest = lax.rem(s + i, ns)
        push(dtw.at[s], dtw.at[s], d_send.at[dest], d_recv.at[s], (dest, t))

    def share_rates():
        for i in range(1, nt):
            peer = lax.rem(t + i, nt)
            wait_in(sums.at[peer], s_recv.at[peer], me)
        total = sums[0]
        for i in range(1, nt):
            total = total + sums[i]
        rates[s] = lax.rsqrt(total * (1.0 / (nt * feats)) + epsilon)
        for i in range(1, ns):
            dest = lax.rem(s + i, ns)
            push(rates.at[s], rates.at[s], r_send.at[dest], r_recv.at[s], (dest, t))

    from_x(0)
    for k in range(1, nz):
        for dz in (-k, k):
            inside(dz, lambda dz=dz: from_z(dz))
        send_weights_at(k)
        if k == 1:
            share_rates()
        if k > 1:
            for dz in (-(k - 1), k - 1):
                inside(dz, lambda dz=dz: from_x(dz))
        if k == 2:
            from_y(0)
    for dz in (-(nz - 1), nz - 1):
        inside(dz, lambda dz=dz: from_x(dz))
    for copy in own_copies:
        copy.wait()

    def weight_ready(source):
        @pl.when(source != s)
        def _():
            wait_in(wgt.at[source], w_recv.at[source], me)
            wait_in(dtw.at[source], d_recv.at[source], me)

        side[source, :, 0:lanes] = wgt[source, :, main:]
        short = dtw[source].astype(jnp.float32)
        short = pltpu.roll(short, lax.rem(short.shape[0] - s * heads, short.shape[0]), 0)
        padded = jnp.concatenate([short, jnp.zeros((lanes - short.shape[0], depth), jnp.float32)], axis=0)
        side[source, :, lanes:] = jnp.transpose(padded).astype(jnp.bfloat16)

    def product(block, part, tiles, put):
        first = part * (nt // 2)
        lhs = jnp.concatenate([tok_at(block, first + i)[...] for i in range(nt // 2)], axis=1)
        source = pl.ds(part * half_w, half_w)
        for n in tiles:
            if n < main:
                rhs = wgt[source, :, n : n + 256]
            else:
                rhs = side[source, :, n - main : n - main + 256]
            rhs = rhs.reshape(half_w * depth, 256)
            put(n, jnp.dot(lhs, rhs, preferred_element_type=jnp.float32))

    @pl.loop(0, half_w)
    def _(i):
        weight_ready(near * half_w + i)

    def begin(block):
        def put(n, value):
            acc[block, :, n : n + 256] = value

        product(block, near, range(0, main + 256, 256), put)

    @pl.loop(0, ns)
    def _(block):
        @pl.when(block != s)
        def _():
            wait_in(rates.at[block], r_recv.at[block], me)

        for r in range(0, rows, lanes):
            row = rates[block, 0:1, r : r + lanes]
            scales_in[block, r : r + lanes, :] = jnp.transpose(jnp.broadcast_to(row, (lanes, lanes)))

    for dz in steps:

        def group(dz=dz):
            if dz != 0:
                from_y(dz)
            from_core(dz, tc)
            from_core(dz, tyc)

            @pl.loop(0, 2)
            def _(flip):
                begin(2 * (z + dz) + flip)

        inside(dz, group)

    @pl.loop(0, half_w)
    def _(i):
        weight_ready((1 - near) * half_w + i)

    def scaled_sum(block, n, value):
        scale = scales_in[block]
        return (acc[block, :, n : n + 256] + value) * jnp.concatenate([scale, scale], axis=1)

    def first_part(block):
        def put(n, value):
            value = scaled_sum(block, n, value)
            bcs[x, block] = value[:, 0:lanes].astype(jnp.bfloat16)
            acc[block, :, main + lanes :] = value[:, lanes:]

        product(block, 1 - near, [main], put)
        push(bcs.at[x, block], bcs.at[x, block], b_send.at[block], b_recv.at[block], (sx, t))

    @pl.loop(0, ns)
    def _(block):
        first_part(block)

    def finish(block):
        def put(n, value):
            acc[block, :, n : n + 256] = scaled_sum(block, n, value)

        product(block, 1 - near, range(0, main, 256), put)

    tail[...] = jnp.zeros_like(tail)
    state[...] = jnp.zeros_like(state)
    column = pl.multiple_of(s * width, lanes)
    tap_count = convx_ref.shape[0]
    group = s // group_devices
    taps_x = [convx_ref[pl.ds(k, 1), pl.ds(column, width)] for k in range(tap_count)]
    taps_x.append(biasx_ref[:, pl.ds(column, width)])
    taps_bc = [convbc_ref[k, pl.ds(group, 1), :] for k in range(tap_count)]
    taps_bc.append(biasbc_ref[pl.ds(group, 1), :])
    head_lanes = lax.broadcasted_iota(jnp.int32, (1, lanes), 1)

    def lane_row(ref):
        row = jnp.zeros((1, lanes), jnp.float32)
        for h in range(heads):
            row = jnp.where(head_lanes == h, ref[s * heads + h], row)
        return row

    dt_bias, decay = lane_row(dt_bias_ref), lane_row(decay_ref)
    out_gain = out_gain_ref[:, pl.ds(column, width)]
    span_rows = lax.broadcasted_iota(jnp.int32, (SPAN, SPAN), 0)
    span_cols = lax.broadcasted_iota(jnp.int32, (SPAN, SPAN), 1)
    causal = span_rows >= span_cols
    lower = jnp.where(causal, 1.0, 0.0)

    def conv(previous, current, taps):
        padded = jnp.concatenate([previous, current], axis=0)
        running = taps[tap_count]
        for k in range(tap_count):
            start = 8 - (tap_count - 1) + k
            running = running + taps[k] * padded[start : start + SPAN]
        return (running * jax.nn.sigmoid(running)).astype(jnp.bfloat16)

    def rounded(block, r, first, size):
        return acc[block, r : r + SPAN, first : first + size].astype(jnp.bfloat16).astype(jnp.float32)

    def span(block, r):
        i = r // SPAN
        x_raw = rounded(block, r, 0, width)
        b_raw = bcs[0, block, r : r + SPAN, :].astype(jnp.float32)
        c_raw = bcs[1, block, r : r + SPAN, :].astype(jnp.float32)
        bc_raw = jnp.concatenate([b_raw, c_raw], axis=1)
        x_conv = conv(tail[:, 0:width], x_raw, taps_x)
        bc_conv = conv(tail[:, width:], bc_raw, taps_bc)
        tail[:, 0:width] = x_raw[SPAN - 8 :]
        tail[:, width:] = bc_raw[SPAN - 8 :]
        b_conv, c_conv = bc_conv[:, 0:lanes], bc_conv[:, lanes:]
        raw = acc[block, r : r + SPAN, main + lanes :] + dt_bias
        dt = jnp.maximum(raw, 0.0) + jnp.log1p(jnp.exp(-jnp.abs(raw)))
        cum = jnp.dot(lower, -dt * decay, precision=lax.Precision.HIGHEST, preferred_element_type=jnp.float32)
        cum_t = jnp.transpose(cum)
        dt_t = jnp.transpose(dt)
        scores = lax.dot_general(c_conv, b_conv, (((1,), (1,)), ((), ())), preferred_element_type=jnp.float32)
        b_t = jnp.transpose(b_conv.astype(jnp.float32)).astype(jnp.bfloat16)
        squares = None
        for h in range(heads):
            x_h = x_conv[:, h * head_dim : (h + 1) * head_dim]
            x_f = x_h.astype(jnp.float32)
            cum_h = cum[:, h : h + 1]
            gap = jnp.where(causal, cum_h - cum_t[h : h + 1, :], -jnp.inf)
            mix = (scores * jnp.exp(gap) * dt_t[h : h + 1, :]).astype(jnp.bfloat16)
            value = jnp.dot(mix, x_h, preferred_element_type=jnp.float32)
            last = cum[SPAN - 1 : SPAN, h : h + 1]
            scaled = (x_f * (jnp.exp(last - cum_h) * dt[:, h : h + 1])).astype(jnp.bfloat16)
            entering = state[h]
            value = value + jnp.exp(cum_h) * jnp.dot(
                c_conv, entering.astype(jnp.bfloat16), preferred_element_type=jnp.float32
            )
            state[h] = jnp.exp(last) * entering + jnp.dot(b_t, scaled, preferred_element_type=jnp.float32)
            value = value + skip_ref[s * heads + h] * x_f
            gate = rounded(block, r, width + h * head_dim, head_dim)
            value = value * (gate * jax.nn.sigmoid(gate))
            square = jnp.sum(value * value, axis=1, keepdims=True)
            squares = square if squares is None else squares + square
            gain = out_gain[:, h * head_dim : (h + 1) * head_dim]
            gated[i, block, :, h * head_dim : (h + 1) * head_dim] = (value * gain).astype(jnp.bfloat16)
        norms[i, block] = as_row(squares)

        @pl.when(block != s)
        def _():
            push(gated.at[i, block], landed.at[i, s], g_send.at[i, block], g_recv.at[i, s], (block, t))
            push(norms.at[i, block], norms_in.at[i, s], n_send.at[i, block], n_recv.at[i, s], (block, t))

        @pl.when(block == s)
        def _():
            landed[i, s] = gated[i, block]
            norms_in[i, s] = norms[i, block]

    def scan(block):
        wait_in(bcs.at[1 - x, block], b_recv.at[block], me)
        for r in range(0, rows, SPAN):
            span(block, r)

    @pl.loop(0, ns - 1)
    def _(block):
        finish(block)
        scan(block)

    finish(ns - 1)

    @pl.loop(0, ns)
    def _(block):
        wait_out(tok_at(block, t), y_send.at[block], me)
        wait_out(tok_at(block, t), core_send.at[0, block], me)
        wait_out(tok_at(block, t), core_send.at[1, block], me)

    for dz in steps:

        def drain(dz=dz):
            zb = z + dz
            if dz <= 0:
                pl.when(z < nz - 1)(lambda: wait_out(tok_at(0, 0), z_up.at[zb], me))
            if dz >= 0:
                pl.when(z > 0)(lambda: wait_out(tok_at(0, 0), z_down.at[zb], me))
            wait_out(tok_at(0, 0), x_send.at[zb], me)

        inside(dz, drain)

    inner = wout_ref.shape[0]
    def fetch(owner):
        return pltpu.make_async_copy(
            wout_ref.at[:, pl.ds(pl.multiple_of(owner * feats, lanes), feats)],
            tok.at[pl.ds(pl.multiple_of(owner * inner, lanes), inner), :],
            own_sem.at[owner],
        )

    for owner in (tyc, ty, tc, t):
        fetch(owner).start()
    scan(ns - 1)

    def inputs(r):
        scales, lhs = [], []
        for g in range(groups):
            total = norms_in[r, g * group_devices]
            for i in range(1, group_devices):
                total = total + norms_in[r, g * group_devices + i]
            scales.append(as_column(lax.rsqrt(total * (1.0 / group_width) + epsilon)))
            lhs.append(jnp.concatenate([landed[r, g * group_devices + i] for i in range(group_devices)], axis=1))
        return scales, lhs

    def partial(r, values, owner):
        @pl.when(r == 0)
        def _():
            fetch(owner).wait()

        scales, lhs = values
        total = None
        for g in range(groups):
            row = pl.multiple_of(owner * inner + g * group_width, lanes)
            term = scales[g] * jnp.dot(lhs[g], tok[pl.ds(row, group_width), :], preferred_element_type=jnp.float32)
            total = term if total is None else total + term
        return total

    def to_core(r, values, slot, owner):
        send_one[r, slot] = partial(r, values, owner).astype(jnp.bfloat16)
        push(send_one.at[r, slot], recv_one.at[r, slot], one_send.at[r, slot], one_recv.at[r, slot], (s, tc))

    @pl.loop(0, rows // SPAN)
    def _(r):
        for i in range(1, ns):
            source = lax.rem(s + i, ns)
            wait_in(landed.at[r, source], g_recv.at[r, source], me)
            wait_in(norms_in.at[r, source], n_recv.at[r, source], me)
        values = inputs(r)
        to_core(r, values, 0, tyc)
        mine = partial(r, values, ty)
        wait_in(recv_one.at[r, 0], one_recv.at[r, 0], me)
        send_two[r] = (mine + recv_one[r, 0].astype(jnp.float32)).astype(jnp.bfloat16)
        push(send_two.at[r], recv_two.at[r], two_send.at[r], two_recv.at[r], (s, ty))

    @pl.loop(0, rows // SPAN)
    def _(r):
        values = inputs(r)
        to_core(r, values, 1, tc)
        mine = partial(r, values, t)
        wait_in(recv_one.at[r, 1], one_recv.at[r, 1], me)
        span = pl.ds(pl.multiple_of(r * SPAN, SPAN), SPAN)
        final[r] = mine + recv_one[r, 1].astype(jnp.float32) + x_ref[span, :].astype(jnp.float32)

    for r in range(rows // SPAN):
        wait_in(recv_two.at[r], two_recv.at[r], me)
        out_ref[r * SPAN : (r + 1) * SPAN, :] = (final[r] + recv_two[r].astype(jnp.float32)).astype(jnp.bfloat16)

    for i in range(1, ns):
        dest = lax.rem(s + i, ns)
        for r in range(rows // SPAN):
            wait_out(gated.at[r, dest], g_send.at[r, dest], me)
            wait_out(norms.at[r, dest], n_send.at[r, dest], me)
        wait_out(wgt.at[dest], w_send.at[dest], me)
        wait_out(dtw.at[dest], d_send.at[dest], me)
        wait_out(rates.at[dest], r_send.at[dest], me)

    @pl.loop(0, ns)
    def _(block):
        wait_out(bcs.at[x, block], b_send.at[block], me)

    for i in range(1, nt):
        wait_out(sums.at[t], s_send.at[lax.rem(t + i, nt)], me)
    for r in range(rows // SPAN):
        for slot in range(2):
            wait_out(send_one.at[r, slot], one_send.at[r, slot], me)
        wait_out(send_two.at[r], two_send.at[r], me)


def spread_heads(ns, nt, *args):
    (hidden_in, norm_gain, w_x, w_z, w_bc, w_dt, dt_bias, decay_rate,
     conv_x, conv_bc, conv_bias_x, conv_bias_bc, skip_d, out_gain, w_out) = args
    rows, feats = hidden_in.shape
    depth, columns = w_x.shape
    width = columns // ns
    heads = decay_rate.shape[0] // ns
    groups, bc_width = w_bc.shape[1], w_bc.shape[2]
    state_dim = bc_width // 2
    head_dim = width // heads
    flat_bc = w_bc.reshape(depth, groups * bc_width)
    hbm = pl.BlockSpec(memory_space=pl.ANY)
    vmem = pl.BlockSpec(memory_space=pltpu.VMEM)
    smem = pl.BlockSpec(memory_space=pltpu.SMEM)
    dma = pltpu.SemaphoreType.DMA
    spans = rows // SPAN
    return pl.pallas_call(
        functools.partial(layer_kernel, (ns, nt, heads)),
        out_shape=jax.ShapeDtypeStruct((rows, feats), jnp.bfloat16),
        in_specs=[vmem, vmem, hbm, hbm, hbm, vmem, vmem, vmem, vmem, vmem, smem, smem, smem, vmem, hbm],
        out_specs=vmem,
        scratch_shapes=[
            pltpu.VMEM((ns * nt * rows, feats), jnp.bfloat16),
            pltpu.VMEM((ns, depth, 2 * width + 128), jnp.bfloat16),
            pltpu.VMEM((ns, depth, 256), jnp.bfloat16),
            pltpu.VMEM((ns, rows, 2 * width + 256), jnp.float32),
            pltpu.VMEM((ns, w_dt.shape[1], depth), jnp.bfloat16),
            pltpu.VMEM((nt, 8, rows), jnp.float32),
            pltpu.VMEM((ns, 8, rows), jnp.float32),
            pltpu.VMEM((ns, rows, 128), jnp.float32),
            pltpu.VMEM((2, ns, rows, 128), jnp.bfloat16),
            pltpu.VMEM((8, width + bc_width), jnp.float32),
            pltpu.VMEM((heads, state_dim, head_dim), jnp.float32),
            pltpu.VMEM((spans, ns, SPAN, width), jnp.bfloat16),
            pltpu.VMEM((spans, ns, 8, SPAN), jnp.float32),
            pltpu.VMEM((spans, ns, SPAN, width), jnp.bfloat16),
            pltpu.VMEM((spans, ns, 8, SPAN), jnp.float32),
            pltpu.VMEM((spans, 2, SPAN, feats), jnp.bfloat16),
            pltpu.VMEM((spans, 2, SPAN, feats), jnp.bfloat16),
            pltpu.VMEM((spans, SPAN, feats), jnp.bfloat16),
            pltpu.VMEM((spans, SPAN, feats), jnp.bfloat16),
            pltpu.VMEM((spans, SPAN, feats), jnp.float32),
            dma((4,)), dma((ns, nt)), dma((ns // 2,)), dma((ns // 2,)), dma((ns // 2,)), dma((ns,)), dma((2, ns)),
            dma((ns,)), dma((ns,)), dma((ns,)), dma((ns,)), dma((nt,)), dma((nt,)), dma((ns,)), dma((ns,)),
            dma((ns,)), dma((ns,)),
            dma((spans, ns)), dma((spans, ns)), dma((spans, ns)), dma((spans, ns)),
            dma((spans, 2)), dma((spans, 2)), dma((spans,)), dma((spans,)),
        ],
        compiler_params=pltpu.CompilerParams(
            collective_id=0, has_side_effects=True, vmem_limit_bytes=63 * 1024 * 1024
        ),
        name="layer",
    )(
        hidden_in, norm_gain.reshape(1, nt * feats), w_x, w_z, flat_bc, w_dt,
        conv_x, conv_bias_x.reshape(1, columns), conv_bc, conv_bias_bc, dt_bias, decay_rate, skip_d,
        out_gain.reshape(1, columns), w_out,
    )


def fits(mesh, args):
    ns, nt = mesh.shape["seq"], mesh.shape["tensor"]
    hidden_in, w_x, w_bc, decay_rate = args[0], args[2], args[4], args[7]
    if nt != 4 or ns % 2 or ns > 8:
        return False
    rows, feats = hidden_in.shape[0] // ns, hidden_in.shape[1] // nt
    groups, heads = w_bc.shape[1] // nt, decay_rate.shape[0] // nt
    if rows % SPAN or feats % 512 or heads % ns or ns % (2 * groups) or ns % 4 or (decay_rate.shape[0] // nt) % 16:
        return False
    width = w_x.shape[1] // (nt * ns)
    state = w_bc.shape[2] // 2
    if args[14].shape[0] // nt > hidden_in.shape[0]:
        return False
    return width % 256 == 0 and state == 128 and width * ns // heads == 128 and rows * hidden_in.shape[1] <= 384 * 4096


def solution(mesh):
    seq, tensor = mesh.shape["seq"], mesh.shape["tensor"]
    in_tail = (
        P("tensor"), P("tensor"), P(None, "tensor"), P(None, "tensor", None), P("tensor"), P("tensor", None),
        P("tensor"), P("tensor"), P("tensor", None),
    )

    def run(*args):
        if fits(mesh, args):
            return jax.shard_map(
                functools.partial(spread_heads, seq, tensor),
                mesh=mesh,
                in_specs=(
                    P("seq", "tensor"), P(), P("seq", "tensor"), P("seq", "tensor"),
                    P("seq", "tensor", None), P("seq", "tensor"),
                ) + in_tail,
                out_specs=P("seq", "tensor"),
                check_vma=False,
            )(*args)
        groups = args[4].shape[1] // tensor
        fold = 2 if groups % 2 == 0 and seq % 2 == 0 else 1
        split = Mesh(
            mesh.devices.reshape(seq // fold, fold, tensor), ("outer", "fold", "tensor")
        )
        both = ("outer", "fold")
        in_specs = (
            P(both, "tensor"), P(), P(both, "tensor"), P(both, "tensor"), P(both, "tensor", None), P(both, "tensor"),
        ) + in_tail
        return jax.shard_map(
            local, mesh=split, in_specs=in_specs, out_specs=P(both, "tensor"), check_vma=False
        )(*args)

    return run
```

```python
import functools

import jax
import jax.numpy as jnp
from jax import lax
from jax.experimental import pallas as pl
from jax.experimental.pallas import tpu as pltpu
from jax.sharding import Mesh, PartitionSpec as P

MESH = pl.DeviceIdType.MESH
SPAN = 128
RING_LIMIT = 8


epsilon = 1e-05


def rms_scale(values, norm_weight):
    return (
        values
        * lax.rsqrt(jnp.mean(values * values, axis=-1, keepdims=True) + epsilon)
        * norm_weight
    )


def causal_conv(padded, weight, bias_row):
    tap_count = weight.shape[0]
    out_length = padded.shape[0] - tap_count + 1
    running = bias_row
    for k in range(tap_count):
        running = running + weight[k] * padded[k : k + out_length].astype(jnp.float32)
    return jax.nn.silu(running).astype(jnp.bfloat16)


def span_terms(x_blocks, b_blocks, c_blocks, log_decay, dt_blocks):
    cum_decay = jnp.cumsum(log_decay, axis=1)
    scores = jnp.einsum("ctgn,csgn->cgts", c_blocks, b_blocks, preferred_element_type=jnp.float32)
    length = x_blocks.shape[1]
    causal_mask = lax.broadcasted_iota(jnp.int32, (length, length), 0) >= lax.broadcasted_iota(
        jnp.int32, (length, length), 1
    )
    cum_rows = jnp.transpose(cum_decay, (0, 2, 3, 1))
    decay_gap = cum_rows[..., :, None] - cum_rows[..., None, :]
    decay_mat = jnp.where(causal_mask, jnp.exp(jnp.where(causal_mask, decay_gap, 0.0)), 0.0)
    dt_cols = jnp.transpose(dt_blocks, (0, 2, 3, 1))[..., None, :]
    mix_weight = (scores[:, :, None] * decay_mat * dt_cols).astype(jnp.bfloat16)
    intra_out = jnp.einsum(
        "cgkts,csgkp->ctgkp", mix_weight, x_blocks, preferred_element_type=jnp.float32
    )
    tail_decay = jnp.exp(cum_decay[:, -1:] - cum_decay) * dt_blocks
    scaled = (x_blocks.astype(jnp.float32) * tail_decay[..., None]).astype(jnp.bfloat16)
    fresh_state = jnp.einsum(
        "csgkp,csgn->cgkpn", scaled, b_blocks, preferred_element_type=jnp.float32
    )
    return (cum_decay, intra_out, fresh_state)


def shifted(block, axis, distance):
    count = lax.axis_size(axis)
    return lax.ppermute(block, axis, [(i, (i + distance) % count) for i in range(count)])


def passed_along(block, axis, distance):
    devices = range(lax.axis_size(axis))
    return lax.ppermute(block, axis, [(i - distance, i) for i in devices if i - distance in devices])


def swapped(block, axis, bit):
    return lax.ppermute(block, axis, [(i, i ^ bit) for i in range(lax.axis_size(axis))])


def ring_pieces(own, axis):
    count = lax.axis_size(axis)
    pieces = [(0, 0, own)]
    ahead, behind = own, own
    for step in range(1, (count - 1) // 2 + 1):
        ahead, behind = shifted(ahead, axis, 1), shifted(behind, axis, -1)
        pieces += [(step, 0, ahead), (count - step, 0, behind)]
    if count % 2 == 0:
        half = own.shape[0] // 2
        pieces += [
            (count // 2, 0, shifted(ahead[:half], axis, 1)),
            (count // 2, half, shifted(behind[half:], axis, -1)),
        ]
    return pieces


def carried_in(total_log, state):
    count, mine = lax.axis_size("outer"), lax.axis_index("outer")
    logs, states = lax.all_gather((total_log, state), "outer")

    def hop(position, running):
        longer = jnp.exp(logs[position])[..., None, None] * running + states[position]
        return jnp.where(position < mine, longer, running)

    return lax.fori_loop(0, count - 1, hop, jnp.zeros_like(state))


def gather_tokens(hidden_in):
    tensor, fold = lax.axis_size("tensor"), lax.axis_size("fold")
    rows, cols = hidden_in.shape
    pieces = [(0, 0, hidden_in)]
    bits = []
    bit = tensor // 2
    while bit > 1:
        bits.append(("tensor", bit))
        bit //= 2
    if fold > 1:
        bits.append(("fold", 1))
    if tensor > 1:
        bits.append(("tensor", 1))
    for axis, bit in bits:
        pieces += [
            (j ^ bit, k, swapped(part, axis, bit)) if axis == "tensor" else (j, k ^ bit, swapped(part, axis, bit))
            for j, k, part in list(pieces)
        ]
    full = jnp.zeros((tensor, rows * fold, cols), hidden_in.dtype)
    me_t, me_f = lax.axis_index("tensor"), lax.axis_index("fold")
    for j, k, part in pieces:
        full = lax.dynamic_update_slice(full, part[None], (me_t ^ j, (me_f ^ k) * rows, 0))
    return full


def scatter_sum(partial, rows, cols):
    tensor, fold = lax.axis_size("tensor"), lax.axis_size("fold")
    me_t, me_f = lax.axis_index("tensor"), lax.axis_index("fold")
    if tensor > 1:
        pairs = partial.reshape(fold * rows, tensor // 2, 2, cols)
        core = me_t % 2
        keep = lax.dynamic_index_in_dim(pairs, core, 2, keepdims=False)
        send = lax.dynamic_index_in_dim(pairs, 1 - core, 2, keepdims=False)
        keep = keep.astype(jnp.float32) + swapped(send.astype(jnp.bfloat16), "tensor", 1).astype(jnp.float32)
    else:
        keep = partial.reshape(fold * rows, 1, cols).astype(jnp.float32)

    def over_fold(value):
        if fold == 1:
            return value
        split = value.reshape(fold, rows, *value.shape[1:])
        mine = lax.dynamic_index_in_dim(split, me_f, 0, keepdims=False)
        other = lax.dynamic_index_in_dim(split, 1 - me_f, 0, keepdims=False)
        return mine + swapped(other.astype(jnp.bfloat16), "fold", 1).astype(jnp.float32)

    def over_high(value):
        count = tensor // 2
        bit = tensor // 2
        while count > 1:
            split = value.reshape(value.shape[0], 2, count // 2, value.shape[-1])
            top = (me_t // bit) % 2
            mine = lax.dynamic_index_in_dim(split, top, 1, keepdims=False)
            other = lax.dynamic_index_in_dim(split, 1 - top, 1, keepdims=False)
            value = mine + swapped(other.astype(jnp.bfloat16), "tensor", bit).astype(jnp.float32)
            count, bit = count // 2, bit // 2
        return value

    half = cols // 2
    first = over_high(over_fold(keep[..., :half]))
    second = over_fold(over_high(keep[..., half:]))
    return jnp.concatenate([first.reshape(rows, half), second.reshape(rows, cols - half)], axis=1)


def local(
    hidden_in,
    norm_gain,
    w_x,
    w_z,
    w_bc,
    w_dt,
    dt_bias,
    decay_rate,
    conv_x,
    conv_bc,
    conv_bias_x,
    conv_bias_bc,
    skip_d,
    out_gain,
    w_out,
):
    fold = lax.axis_size("fold")
    me_f = lax.axis_index("fold")
    me_o = lax.axis_index("outer")
    outer = lax.axis_size("outer")

    def part(value, axis, which=None):
        size = value.shape[axis] // fold
        which = me_f if which is None else which
        return lax.dynamic_slice_in_dim(value, which * size, size, axis)

    depth = w_x.shape[0]
    groups = w_bc.shape[1] // fold
    bc_width = w_bc.shape[2]
    bc_flat = w_bc.reshape(depth, w_bc.shape[1] * bc_width)
    state_dim = bc_width // 2
    head_count = decay_rate.shape[0] // fold
    inner_width = w_x.shape[1] // fold
    head_dim = inner_width // head_count
    per_group = head_count // groups

    def weights(which):
        side = jnp.concatenate([part(bc_flat, 1, which), part(w_dt, 1, which)], axis=1)
        return [jnp.concatenate([part(w_x, 1, which), side], axis=1), part(w_z, 1, which)]

    own = weights(me_f)
    other = [swapped(block, "fold", 1) for block in weights(1 - me_f)] if fold > 1 else []
    gathered = gather_tokens(hidden_in)
    blocks, row_count, width = gathered.shape
    values = gathered.astype(jnp.float32)
    scale = lax.rsqrt(jnp.mean(values * values, axis=(0, 2), keepdims=True) + epsilon)
    normed = (values * scale * norm_gain.reshape(blocks, 1, width)).astype(jnp.bfloat16)
    per_block = max(width // depth, 1)
    if outer <= RING_LIMIT:
        normed = normed.reshape(blocks, row_count, per_block, width // per_block)
        normed = jnp.transpose(normed, (0, 2, 1, 3)).reshape(blocks * per_block, row_count, depth)
    else:
        normed = jnp.transpose(normed, (1, 0, 2)).reshape(row_count, blocks * width)
    rim_rows = conv_x.shape[0] - 1

    def projected(index):
        total = None
        if outer > RING_LIMIT:
            rows = lax.all_gather(own[index], "outer")
            if fold > 1:
                theirs = lax.all_gather(other[index], "outer")
                first, second = jnp.where(me_f == 0, rows, theirs), jnp.where(me_f == 0, theirs, rows)
                rows = jnp.stack([first, second], axis=1)
            rows = rows.reshape(normed.shape[1], own[index].shape[1])
            return jnp.dot(normed, rows, preferred_element_type=jnp.float32)
        for k, block in enumerate([own, other] if fold > 1 else [own]):
            for behind, offset, piece in ring_pieces(block[index], "outer"):
                owner = (me_o - behind + outer) % outer
                lhs = lax.dynamic_index_in_dim(normed, owner * fold + (me_f ^ k), 0, keepdims=False)
                lhs = lhs[:, offset : offset + piece.shape[0]]
                term = jnp.dot(lhs, piece, preferred_element_type=jnp.float32)
                total = term if total is None else total + term
        return total

    first = projected(0)
    proj_x = first[:, :inner_width].astype(jnp.bfloat16)
    side = first[:, inner_width:]
    dt_raw = side[:, groups * bc_width :]
    proj_bc = side[:, : groups * bc_width].astype(jnp.bfloat16)
    gate_z = projected(1).astype(jnp.bfloat16)
    edge_x, edge_bc = passed_along(
        (proj_x[row_count - rim_rows :], proj_bc[row_count - rim_rows :]), "outer", 1
    )
    padded_x = jnp.concatenate([edge_x, proj_x], axis=0)
    padded_bc = jnp.concatenate([edge_bc, proj_bc], axis=0)
    dt_vals = jax.nn.softplus(dt_raw + part(dt_bias, 0))
    x_conv = causal_conv(padded_x, part(conv_x, 1), part(conv_bias_x, 0))
    bc_conv = causal_conv(
        padded_bc,
        part(conv_bc, 1).reshape(conv_bc.shape[0], groups * bc_width),
        part(conv_bias_bc, 0).reshape(groups * bc_width),
    ).reshape(row_count, groups, bc_width)
    span_count = row_count // SPAN
    x_blocks = x_conv.reshape(span_count, SPAN, groups, per_group, head_dim)
    b_blocks = bc_conv[..., :state_dim].reshape(span_count, SPAN, groups, state_dim)
    c_blocks = bc_conv[..., state_dim:].reshape(span_count, SPAN, groups, state_dim)
    log_decay = (-dt_vals * part(decay_rate, 0)).reshape(span_count, SPAN, groups, per_group)
    dt_blocks = dt_vals.reshape(span_count, SPAN, groups, per_group)
    cum_decay, intra_out, fresh_state = span_terms(
        x_blocks, b_blocks, c_blocks, log_decay, dt_blocks
    )
    block_totals = cum_decay[:, -1]
    state = jnp.zeros((groups, per_group, head_dim, state_dim), jnp.float32)
    entering = []
    for i in range(span_count):
        entering.append(state)
        state = jnp.exp(block_totals[i])[..., None, None] * state + fresh_state[i]
    local_enter = jnp.stack(entering)
    before_log = jnp.cumsum(block_totals, axis=0) - block_totals
    total_log = jnp.sum(block_totals, axis=0)
    if outer > RING_LIMIT:
        incoming = carried_in(total_log, state)
    else:
        incoming = jnp.zeros_like(state)
        log_between = jnp.zeros_like(total_log)
        for distance in range(1, outer):
            arrived = passed_along(state, "outer", distance)
            incoming = incoming + jnp.exp(log_between)[..., None, None] * arrived
            log_between = log_between + passed_along(total_log, "outer", distance)
    enter_state = local_enter + jnp.exp(before_log)[..., None, None] * incoming[None]
    inter_out = jnp.exp(cum_decay)[..., None] * jnp.einsum(
        "ctgn,cgkpn->ctgkp", c_blocks, enter_state.astype(jnp.bfloat16), preferred_element_type=jnp.float32
    )
    skip_heads = part(skip_d, 0).reshape(groups, per_group)[..., None]
    ssm_out = (intra_out + inter_out + skip_heads * x_blocks.astype(jnp.float32)).reshape(
        row_count, inner_width
    )
    gated_out = ssm_out * jax.nn.silu(gate_z.astype(jnp.float32))
    grouped = gated_out.reshape(row_count, groups, inner_width // groups)
    normed_y = (
        rms_scale(grouped, part(out_gain, 0).reshape(groups, inner_width // groups))
        .reshape(row_count, inner_width)
        .astype(jnp.bfloat16)
    )
    partial = jnp.dot(normed_y, part(w_out, 0), preferred_element_type=jnp.float32)
    summed = scatter_sum(partial, *hidden_in.shape)
    return (hidden_in.astype(jnp.float32) + summed).astype(jnp.bfloat16)


def wait_in(dst, sem, me):
    pltpu.make_async_remote_copy(
        src_ref=dst, dst_ref=dst, send_sem=sem, recv_sem=sem, device_id=me, device_id_type=MESH
    ).wait_recv()


def wait_out(src, sem, me):
    pltpu.make_async_remote_copy(
        src_ref=src, dst_ref=src, send_sem=sem, recv_sem=sem, device_id=me, device_id_type=MESH
    ).wait_send()


def push(src, dst, send_sem, recv_sem, device):
    pltpu.make_async_remote_copy(
        src_ref=src, dst_ref=dst, send_sem=send_sem, recv_sem=recv_sem, device_id=device, device_id_type=MESH
    ).start()


def greet(partners):
    barrier = pltpu.get_barrier_semaphore()
    for device in partners:
        pl.semaphore_signal(barrier, inc=1, device_id=device, device_id_type=MESH)
    pl.semaphore_wait(barrier, len(partners))


def guarded(condition, action):
    if condition is None:
        action()
    else:
        pl.when(condition)(action)


def as_column(row):
    return jnp.transpose(jnp.broadcast_to(row[0:1], (row.shape[1], row.shape[1])))[:, 0:1]


def as_row(column):
    return jnp.transpose(jnp.broadcast_to(column, (column.shape[0], column.shape[0])))[0:8]


def layer_kernel(
    dims,
    x_ref, gain_ref, wx_ref, wz_ref, wbc_ref, wdt_ref,
    convx_ref, biasx_ref, convbc_ref, biasbc_ref, dt_bias_ref, decay_ref, skip_ref, out_gain_ref, wout_ref,
    out_ref,
    tok, wgt, side, acc, dtw, sums, rates, scales_in, bcs,
    tail, state, gated, norms, landed, norms_in, send_one, recv_one, send_two, recv_two, final,
    own_sem, tok_recv, z_up, z_down, x_send, y_send, core_send,
    w_send, w_recv, d_send, d_recv, s_send, s_recv, b_send, b_recv,
    r_send, r_recv, g_send, g_recv, n_send, n_recv, one_send, one_recv, two_send, two_recv,
):
    ns, nt, heads = dims
    nz = ns // 2
    rows, feats = x_ref.shape
    depth = wx_ref.shape[0]
    width = wx_ref.shape[1] // ns
    head_dim = width // heads
    lanes = 128
    s, t = lax.axis_index("seq"), lax.axis_index("tensor")
    z, x = s // 2, s % 2
    zz = nz - 1 - z
    y, core = t // 2, t % 2
    me = (s, t)
    sx = 2 * z + 1 - x
    ty = 2 * (1 - y) + core
    tc = 2 * y + 1 - core
    tyc = 2 * (1 - y) + 1 - core
    half_w = ns // 2
    near = z // (nz // 2)
    main = 2 * width
    groups = convbc_ref.shape[1]
    group_devices = ns // groups
    group_width = group_devices * width

    partners = [(lax.rem(s + i, ns), t) for i in range(1, ns)]
    partners += [(s, lax.rem(t + i, nt)) for i in range(1, nt)]
    greet(partners)

    def weight_parts(dest):
        group, half = dest // group_devices, dest % 2
        column = pl.multiple_of(dest * width, lanes)
        third = pl.multiple_of((group * 2 + half) * lanes, lanes)
        return [
            (wx_ref.at[:, pl.ds(column, width)], 0, width),
            (wz_ref.at[:, pl.ds(column, width)], width, width),
            (wbc_ref.at[:, pl.ds(third, lanes)], main, lanes),
        ]

    def send_weights(dest, which=(0, 1, 2)):
        parts = weight_parts(dest)
        for src, lane, size in [parts[i] for i in which]:
            push(src, wgt.at[s, :, pl.ds(lane, size)], w_send.at[dest], w_recv.at[s], (dest, t))

    pair = z + 1 - 2 * (z % 2)
    other = z - 1 + 2 * (z % 2)

    def across(flip):
        @pl.when((other >= 0) & (other < nz))
        def _():
            send_weights(2 * other + flip)

    def send_plane(plane):
        send_weights(2 * plane + x)
        send_weights(2 * plane + 1 - x)

    def send_pair():
        send_weights(2 * pair + x, (0, 1))
        send_weights(2 * pair + 1 - x)

    def send_weights_at(k):
        if k == 0:
            send_weights(sx)
        if k == 1:
            pl.when(z * zz == 0)(send_pair)
            across(x)
            across(1 - x)
        if k == min(2, nz - 1):
            pl.when(z * zz > 0)(send_pair)
            for plane in range(2, nz):
                pl.when(z < plane - 1)(lambda: send_plane(plane))
                pl.when(zz < plane - 1)(lambda: send_plane(nz - 1 - plane))

    def inside(dz, action):
        if dz == 0:
            action()
        elif dz > 0:
            pl.when(z + dz < nz)(action)
        else:
            pl.when(z + dz >= 0)(action)

    own_copies = [
        pltpu.make_async_copy(src, wgt.at[s, :, pl.ds(lane, size)], own_sem.at[i])
        for i, (src, lane, size) in enumerate(weight_parts(s))
    ]
    send_weights(2 * pair + x, (2,))
    for copy in own_copies:
        copy.start()
    gain = gain_ref[:, pl.ds(pl.multiple_of(t * feats, lanes), feats)]

    def tok_at(si, ti):
        return tok.at[pl.ds(pl.multiple_of((si * nt + ti) * rows, lanes), rows), :]

    for r in range(0, rows, lanes):
        values = x_ref[r : r + lanes, :].astype(jnp.float32)
        sums[t, :, r : r + lanes] = as_row(jnp.sum(values * values, axis=1, keepdims=True))
        row = pl.multiple_of((s * nt + t) * rows + r, lanes)
        tok[pl.ds(row, lanes), :] = (values * gain).astype(jnp.bfloat16)
    dtw[s] = jnp.transpose(wdt_ref[...].astype(jnp.float32)).astype(jnp.bfloat16)

    def send_tok(si, ti, send_sem, device):
        push(tok_at(si, ti), tok_at(si, ti), send_sem, tok_recv.at[si, ti], device)

    def wait_tok(si, ti):
        wait_in(tok_at(si, ti), tok_recv.at[si, ti], me)

    def from_z(dz):
        zb = z + dz
        block = 2 * zb + x
        if dz != 0:
            wait_tok(block, t)
        if dz <= 0:
            pl.when(z < nz - 1)(lambda: send_tok(block, t, z_up.at[zb], (s + 2, t)))
        if dz >= 0:
            pl.when(z > 0)(lambda: send_tok(block, t, z_down.at[zb], (s - 2, t)))
        send_tok(block, t, x_send.at[zb], (sx, t))
        send_tok(block, t, y_send.at[block], (s, ty))
        send_tok(block, t, core_send.at[0, block], (s, tc))

    def from_x(dz):
        block = 2 * (z + dz) + 1 - x
        wait_tok(block, t)
        send_tok(block, t, y_send.at[block], (s, ty))
        send_tok(block, t, core_send.at[0, block], (s, tc))

    def from_y(dz):
        for flip in (x, 1 - x):
            block = 2 * (z + dz) + flip
            wait_tok(block, ty)
            send_tok(block, ty, core_send.at[1, block], (s, tc))

    def from_core(dz, which):
        for flip in (x, 1 - x):
            wait_tok(2 * (z + dz) + flip, which)

    steps = [0]
    for k in range(1, nz):
        steps += [-k, k]

    for i in range(1, nt):
        peer = lax.rem(t + i, nt)
        push(sums.at[t], sums.at[t], s_send.at[peer], s_recv.at[t], (s, peer))
    from_z(0)
    send_weights_at(0)
    for i in range(1, ns):
        dest = lax.rem(s + i, ns)
        push(dtw.at[s], dtw.at[s], d_send.at[dest], d_recv.at[s], (dest, t))

    def share_rates():
        for i in range(1, nt):
            peer = lax.rem(t + i, nt)
            wait_in(sums.at[peer], s_recv.at[peer], me)
        total = sums[0]
        for i in range(1, nt):
            total = total + sums[i]
        rates[s] = lax.rsqrt(total * (1.0 / (nt * feats)) + epsilon)
        for i in range(1, ns):
            dest = lax.rem(s + i, ns)
            push(rates.at[s], rates.at[s], r_send.at[dest], r_recv.at[s], (dest, t))

    from_x(0)
    for k in range(1, nz):
        for dz in (-k, k):
            inside(dz, lambda dz=dz: from_z(dz))
        send_weights_at(k)
        if k == 1:
            share_rates()
        if k > 1:
            for dz in (-(k - 1), k - 1):
                inside(dz, lambda dz=dz: from_x(dz))
        if k == 2:
            from_y(0)
    for dz in (-(nz - 1), nz - 1):
        inside(dz, lambda dz=dz: from_x(dz))
    for copy in own_copies:
        copy.wait()

    def weight_ready(source):
        @pl.when(source != s)
        def _():
            wait_in(wgt.at[source], w_recv.at[source], me)
            wait_in(dtw.at[source], d_recv.at[source], me)

        side[source, :, 0:lanes] = wgt[source, :, main:]
        short = dtw[source].astype(jnp.float32)
        short = pltpu.roll(short, lax.rem(short.shape[0] - s * heads, short.shape[0]), 0)
        padded = jnp.concatenate([short, jnp.zeros((lanes - short.shape[0], depth), jnp.float32)], axis=0)
        side[source, :, lanes:] = jnp.transpose(padded).astype(jnp.bfloat16)

    def product(block, part, tiles, put):
        first = part * (nt // 2)
        lhs = jnp.concatenate([tok_at(block, first + i)[...] for i in range(nt // 2)], axis=1)
        source = pl.ds(part * half_w, half_w)
        for n in tiles:
            if n < main:
                rhs = wgt[source, :, n : n + 256]
            else:
                rhs = side[source, :, n - main : n - main + 256]
            rhs = rhs.reshape(half_w * depth, 256)
            put(n, jnp.dot(lhs, rhs, preferred_element_type=jnp.float32))

    @pl.loop(0, half_w)
    def _(i):
        weight_ready(near * half_w + i)

    def begin(block):
        def put(n, value):
            acc[block, :, n : n + 256] = value

        product(block, near, range(0, main + 256, 256), put)

    @pl.loop(0, ns)
    def _(block):
        @pl.when(block != s)
        def _():
            wait_in(rates.at[block], r_recv.at[block], me)

        for r in range(0, rows, lanes):
            row = rates[block, 0:1, r : r + lanes]
            scales_in[block, r : r + lanes, :] = jnp.transpose(jnp.broadcast_to(row, (lanes, lanes)))

    for dz in steps:

        def group(dz=dz):
            if dz != 0:
                from_y(dz)
            from_core(dz, tc)
            from_core(dz, tyc)

            @pl.loop(0, 2)
            def _(flip):
                begin(2 * (z + dz) + flip)

        inside(dz, group)

    @pl.loop(0, half_w)
    def _(i):
        weight_ready((1 - near) * half_w + i)

    def scaled_sum(block, n, value):
        scale = scales_in[block]
        return (acc[block, :, n : n + 256] + value) * jnp.concatenate([scale, scale], axis=1)

    def first_part(block):
        def put(n, value):
            value = scaled_sum(block, n, value)
            bcs[x, block] = value[:, 0:lanes].astype(jnp.bfloat16)
            acc[block, :, main + lanes :] = value[:, lanes:]

        product(block, 1 - near, [main], put)
        push(bcs.at[x, block], bcs.at[x, block], b_send.at[block], b_recv.at[block], (sx, t))

    @pl.loop(0, ns)
    def _(block):
        first_part(block)

    def finish(block):
        def put(n, value):
            acc[block, :, n : n + 256] = scaled_sum(block, n, value)

        product(block, 1 - near, range(0, main, 256), put)

    tail[...] = jnp.zeros_like(tail)
    state[...] = jnp.zeros_like(state)
    column = pl.multiple_of(s * width, lanes)
    tap_count = convx_ref.shape[0]
    group = s // group_devices
    taps_x = [convx_ref[pl.ds(k, 1), pl.ds(column, width)] for k in range(tap_count)]
    taps_x.append(biasx_ref[:, pl.ds(column, width)])
    taps_bc = [convbc_ref[k, pl.ds(group, 1), :] for k in range(tap_count)]
    taps_bc.append(biasbc_ref[pl.ds(group, 1), :])
    head_lanes = lax.broadcasted_iota(jnp.int32, (1, lanes), 1)

    def lane_row(ref):
        row = jnp.zeros((1, lanes), jnp.float32)
        for h in range(heads):
            row = jnp.where(head_lanes == h, ref[s * heads + h], row)
        return row

    dt_bias, decay = lane_row(dt_bias_ref), lane_row(decay_ref)
    out_gain = out_gain_ref[:, pl.ds(column, width)]
    span_rows = lax.broadcasted_iota(jnp.int32, (SPAN, SPAN), 0)
    span_cols = lax.broadcasted_iota(jnp.int32, (SPAN, SPAN), 1)
    causal = span_rows >= span_cols
    lower = jnp.where(causal, 1.0, 0.0)

    def conv(previous, current, taps):
        padded = jnp.concatenate([previous, current], axis=0)
        running = taps[tap_count]
        for k in range(tap_count):
            start = 8 - (tap_count - 1) + k
            running = running + taps[k] * padded[start : start + SPAN]
        return (running * jax.nn.sigmoid(running)).astype(jnp.bfloat16)

    def rounded(block, r, first, size):
        return acc[block, r : r + SPAN, first : first + size].astype(jnp.bfloat16).astype(jnp.float32)

    def span(block, r):
        i = r // SPAN
        x_raw = rounded(block, r, 0, width)
        b_raw = bcs[0, block, r : r + SPAN, :].astype(jnp.float32)
        c_raw = bcs[1, block, r : r + SPAN, :].astype(jnp.float32)
        bc_raw = jnp.concatenate([b_raw, c_raw], axis=1)
        x_conv = conv(tail[:, 0:width], x_raw, taps_x)
        bc_conv = conv(tail[:, width:], bc_raw, taps_bc)
        tail[:, 0:width] = x_raw[SPAN - 8 :]
        tail[:, width:] = bc_raw[SPAN - 8 :]
        b_conv, c_conv = bc_conv[:, 0:lanes], bc_conv[:, lanes:]
        raw = acc[block, r : r + SPAN, main + lanes :] + dt_bias
        dt = jnp.maximum(raw, 0.0) + jnp.log1p(jnp.exp(-jnp.abs(raw)))
        cum = jnp.dot(lower, -dt * decay, precision=lax.Precision.HIGHEST, preferred_element_type=jnp.float32)
        cum_t = jnp.transpose(cum)
        dt_t = jnp.transpose(dt)
        scores = lax.dot_general(c_conv, b_conv, (((1,), (1,)), ((), ())), preferred_element_type=jnp.float32)
        b_t = jnp.transpose(b_conv.astype(jnp.float32)).astype(jnp.bfloat16)
        squares = None
        for h in range(heads):
            x_h = x_conv[:, h * head_dim : (h + 1) * head_dim]
            x_f = x_h.astype(jnp.float32)
            cum_h = cum[:, h : h + 1]
            gap = jnp.where(causal, cum_h - cum_t[h : h + 1, :], -jnp.inf)
            mix = (scores * jnp.exp(gap) * dt_t[h : h + 1, :]).astype(jnp.bfloat16)
            value = jnp.dot(mix, x_h, preferred_element_type=jnp.float32)
            last = cum[SPAN - 1 : SPAN, h : h + 1]
            scaled = (x_f * (jnp.exp(last - cum_h) * dt[:, h : h + 1])).astype(jnp.bfloat16)
            entering = state[h]
            value = value + jnp.exp(cum_h) * jnp.dot(
                c_conv, entering.astype(jnp.bfloat16), preferred_element_type=jnp.float32
            )
            state[h] = jnp.exp(last) * entering + jnp.dot(b_t, scaled, preferred_element_type=jnp.float32)
            value = value + skip_ref[s * heads + h] * x_f
            gate = rounded(block, r, width + h * head_dim, head_dim)
            value = value * (gate * jax.nn.sigmoid(gate))
            square = jnp.sum(value * value, axis=1, keepdims=True)
            squares = square if squares is None else squares + square
            gain = out_gain[:, h * head_dim : (h + 1) * head_dim]
            gated[i, block, :, h * head_dim : (h + 1) * head_dim] = (value * gain).astype(jnp.bfloat16)
        norms[i, block] = as_row(squares)

        @pl.when(block != s)
        def _():
            push(gated.at[i, block], landed.at[i, s], g_send.at[i, block], g_recv.at[i, s], (block, t))
            push(norms.at[i, block], norms_in.at[i, s], n_send.at[i, block], n_recv.at[i, s], (block, t))

        @pl.when(block == s)
        def _():
            landed[i, s] = gated[i, block]
            norms_in[i, s] = norms[i, block]

    def scan(block):
        wait_in(bcs.at[1 - x, block], b_recv.at[block], me)
        for r in range(0, rows, SPAN):
            span(block, r)

    @pl.loop(0, ns - 1)
    def _(block):
        finish(block)
        scan(block)

    finish(ns - 1)

    @pl.loop(0, ns)
    def _(block):
        wait_out(tok_at(block, t), y_send.at[block], me)
        wait_out(tok_at(block, t), core_send.at[0, block], me)
        wait_out(tok_at(block, t), core_send.at[1, block], me)

    for dz in steps:

        def drain(dz=dz):
            zb = z + dz
            if dz <= 0:
                pl.when(z < nz - 1)(lambda: wait_out(tok_at(0, 0), z_up.at[zb], me))
            if dz >= 0:
                pl.when(z > 0)(lambda: wait_out(tok_at(0, 0), z_down.at[zb], me))
            wait_out(tok_at(0, 0), x_send.at[zb], me)

        inside(dz, drain)

    inner = wout_ref.shape[0]
    def fetch(owner):
        return pltpu.make_async_copy(
            wout_ref.at[:, pl.ds(pl.multiple_of(owner * feats, lanes), feats)],
            tok.at[pl.ds(pl.multiple_of(owner * inner, lanes), inner), :],
            own_sem.at[owner],
        )

    for owner in (tyc, ty, tc, t):
        fetch(owner).start()
    scan(ns - 1)

    def inputs(r):
        scales, lhs = [], []
        for g in range(groups):
            total = norms_in[r, g * group_devices]
            for i in range(1, group_devices):
                total = total + norms_in[r, g * group_devices + i]
            scales.append(as_column(lax.rsqrt(total * (1.0 / group_width) + epsilon)))
            lhs.append(jnp.concatenate([landed[r, g * group_devices + i] for i in range(group_devices)], axis=1))
        return scales, lhs

    def partial(r, values, owner):
        @pl.when(r == 0)
        def _():
            fetch(owner).wait()

        scales, lhs = values
        total = None
        for g in range(groups):
            row = pl.multiple_of(owner * inner + g * group_width, lanes)
            term = scales[g] * jnp.dot(lhs[g], tok[pl.ds(row, group_width), :], preferred_element_type=jnp.float32)
            total = term if total is None else total + term
        return total

    def to_core(r, values, slot, owner):
        send_one[r, slot] = partial(r, values, owner).astype(jnp.bfloat16)
        push(send_one.at[r, slot], recv_one.at[r, slot], one_send.at[r, slot], one_recv.at[r, slot], (s, tc))

    @pl.loop(0, rows // SPAN)
    def _(r):
        for i in range(1, ns):
            source = lax.rem(s + i, ns)
            wait_in(landed.at[r, source], g_recv.at[r, source], me)
            wait_in(norms_in.at[r, source], n_recv.at[r, source], me)
        values = inputs(r)
        to_core(r, values, 0, tyc)
        mine = partial(r, values, ty)
        wait_in(recv_one.at[r, 0], one_recv.at[r, 0], me)
        send_two[r] = (mine + recv_one[r, 0].astype(jnp.float32)).astype(jnp.bfloat16)
        push(send_two.at[r], recv_two.at[r], two_send.at[r], two_recv.at[r], (s, ty))

    @pl.loop(0, rows // SPAN)
    def _(r):
        values = inputs(r)
        to_core(r, values, 1, tc)
        mine = partial(r, values, t)
        wait_in(recv_one.at[r, 1], one_recv.at[r, 1], me)
        span = pl.ds(pl.multiple_of(r * SPAN, SPAN), SPAN)
        final[r] = mine + recv_one[r, 1].astype(jnp.float32) + x_ref[span, :].astype(jnp.float32)

    for r in range(rows // SPAN):
        wait_in(recv_two.at[r], two_recv.at[r], me)
        out_ref[r * SPAN : (r + 1) * SPAN, :] = (final[r] + recv_two[r].astype(jnp.float32)).astype(jnp.bfloat16)

    for i in range(1, ns):
        dest = lax.rem(s + i, ns)
        for r in range(rows // SPAN):
            wait_out(gated.at[r, dest], g_send.at[r, dest], me)
            wait_out(norms.at[r, dest], n_send.at[r, dest], me)
        wait_out(wgt.at[dest], w_send.at[dest], me)
        wait_out(dtw.at[dest], d_send.at[dest], me)
        wait_out(rates.at[dest], r_send.at[dest], me)

    @pl.loop(0, ns)
    def _(block):
        wait_out(bcs.at[x, block], b_send.at[block], me)

    for i in range(1, nt):
        wait_out(sums.at[t], s_send.at[lax.rem(t + i, nt)], me)
    for r in range(rows // SPAN):
        for slot in range(2):
            wait_out(send_one.at[r, slot], one_send.at[r, slot], me)
        wait_out(send_two.at[r], two_send.at[r], me)


def spread_heads(ns, nt, *args):
    (hidden_in, norm_gain, w_x, w_z, w_bc, w_dt, dt_bias, decay_rate,
     conv_x, conv_bc, conv_bias_x, conv_bias_bc, skip_d, out_gain, w_out) = args
    rows, feats = hidden_in.shape
    depth, columns = w_x.shape
    width = columns // ns
    heads = decay_rate.shape[0] // ns
    groups, bc_width = w_bc.shape[1], w_bc.shape[2]
    state_dim = bc_width // 2
    head_dim = width // heads
    flat_bc = w_bc.reshape(depth, groups * bc_width)
    hbm = pl.BlockSpec(memory_space=pl.ANY)
    vmem = pl.BlockSpec(memory_space=pltpu.VMEM)
    smem = pl.BlockSpec(memory_space=pltpu.SMEM)
    dma = pltpu.SemaphoreType.DMA
    spans = rows // SPAN
    return pl.pallas_call(
        functools.partial(layer_kernel, (ns, nt, heads)),
        out_shape=jax.ShapeDtypeStruct((rows, feats), jnp.bfloat16),
        in_specs=[vmem, vmem, hbm, hbm, hbm, vmem, vmem, vmem, vmem, vmem, smem, smem, smem, vmem, hbm],
        out_specs=vmem,
        scratch_shapes=[
            pltpu.VMEM((ns * nt * rows, feats), jnp.bfloat16),
            pltpu.VMEM((ns, depth, 2 * width + 128), jnp.bfloat16),
            pltpu.VMEM((ns, depth, 256), jnp.bfloat16),
            pltpu.VMEM((ns, rows, 2 * width + 256), jnp.float32),
            pltpu.VMEM((ns, w_dt.shape[1], depth), jnp.bfloat16),
            pltpu.VMEM((nt, 8, rows), jnp.float32),
            pltpu.VMEM((ns, 8, rows), jnp.float32),
            pltpu.VMEM((ns, rows, 128), jnp.float32),
            pltpu.VMEM((2, ns, rows, 128), jnp.bfloat16),
            pltpu.VMEM((8, width + bc_width), jnp.float32),
            pltpu.VMEM((heads, state_dim, head_dim), jnp.float32),
            pltpu.VMEM((spans, ns, SPAN, width), jnp.bfloat16),
            pltpu.VMEM((spans, ns, 8, SPAN), jnp.float32),
            pltpu.VMEM((spans, ns, SPAN, width), jnp.bfloat16),
            pltpu.VMEM((spans, ns, 8, SPAN), jnp.float32),
            pltpu.VMEM((spans, 2, SPAN, feats), jnp.bfloat16),
            pltpu.VMEM((spans, 2, SPAN, feats), jnp.bfloat16),
            pltpu.VMEM((spans, SPAN, feats), jnp.bfloat16),
            pltpu.VMEM((spans, SPAN, feats), jnp.bfloat16),
            pltpu.VMEM((spans, SPAN, feats), jnp.float32),
            dma((4,)), dma((ns, nt)), dma((ns // 2,)), dma((ns // 2,)), dma((ns // 2,)), dma((ns,)), dma((2, ns)),
            dma((ns,)), dma((ns,)), dma((ns,)), dma((ns,)), dma((nt,)), dma((nt,)), dma((ns,)), dma((ns,)),
            dma((ns,)), dma((ns,)),
            dma((spans, ns)), dma((spans, ns)), dma((spans, ns)), dma((spans, ns)),
            dma((spans, 2)), dma((spans, 2)), dma((spans,)), dma((spans,)),
        ],
        compiler_params=pltpu.CompilerParams(
            collective_id=0, has_side_effects=True, vmem_limit_bytes=63 * 1024 * 1024
        ),
        name="layer",
    )(
        hidden_in, norm_gain.reshape(1, nt * feats), w_x, w_z, flat_bc, w_dt,
        conv_x, conv_bias_x.reshape(1, columns), conv_bc, conv_bias_bc, dt_bias, decay_rate, skip_d,
        out_gain.reshape(1, columns), w_out,
    )


def fits(mesh, args):
    ns, nt = mesh.shape["seq"], mesh.shape["tensor"]
    hidden_in, w_x, w_bc, decay_rate = args[0], args[2], args[4], args[7]
    if nt != 4 or ns % 2 or ns > 8:
        return False
    rows, feats = hidden_in.shape[0] // ns, hidden_in.shape[1] // nt
    groups, heads = w_bc.shape[1] // nt, decay_rate.shape[0] // nt
    if rows % SPAN or feats % 512 or heads % ns or ns % (2 * groups) or ns % 4 or (decay_rate.shape[0] // nt) % 16:
        return False
    width = w_x.shape[1] // (nt * ns)
    state = w_bc.shape[2] // 2
    if args[14].shape[0] // nt > hidden_in.shape[0]:
        return False
    return width % 256 == 0 and state == 128 and width * ns // heads == 128 and rows * hidden_in.shape[1] <= 384 * 4096


def solution(mesh):
    seq, tensor = mesh.shape["seq"], mesh.shape["tensor"]
    in_tail = (
        P("tensor"), P("tensor"), P(None, "tensor"), P(None, "tensor", None), P("tensor"), P("tensor", None),
        P("tensor"), P("tensor"), P("tensor", None),
    )

    def run(*args):
        if fits(mesh, args):
            return jax.shard_map(
                functools.partial(spread_heads, seq, tensor),
                mesh=mesh,
                in_specs=(
                    P("seq", "tensor"), P(), P("seq", "tensor"), P("seq", "tensor"),
                    P("seq", "tensor", None), P("seq", "tensor"),
                ) + in_tail,
                out_specs=P("seq", "tensor"),
                check_vma=False,
            )(*args)
        groups = args[4].shape[1] // tensor
        fold = 2 if groups % 2 == 0 and seq % 2 == 0 else 1
        split = Mesh(
            mesh.devices.reshape(seq // fold, fold, tensor), ("outer", "fold", "tensor")
        )
        both = ("outer", "fold")
        in_specs = (
            P(both, "tensor"), P(), P(both, "tensor"), P(both, "tensor"), P(both, "tensor", None), P(both, "tensor"),
        ) + in_tail
        return jax.shard_map(
            local, mesh=split, in_specs=in_specs, out_specs=P(both, "tensor"), check_vma=False
        )(*args)

    return run
```
